32 devices in a mesh: elem: 16 (over z, y, x), param: 2 (over core).
Axes of the slice: x: 2, y: 2, z: 4, core: 2. Of those that a mesh axis runs over, the one named last changes fastest.
Arguments:
- coords: bfloat16 [8, 300], P('param'), may hold values from -6 to 6
- basis_rows: bfloat16 [3, 300, 4096], P(None, None, 'elem'), may hold values from -0.375 to 0.375
- connectivity: int32 [4096, 8], P(('elem', 'param')), may hold values from 0 to 319, as said below
- modulus: float32 [4096], P(('elem', 'param')), may hold values from 0.5 to 15
- stiffness: float32 [24, 24], replicated, may hold values from -1.25 to 1.25
Outputs:
- training: bfloat16 [8, 300, 4096], P(None, None, ('elem', 'param'))
- target: float32 [8, 300], replicated
The draws below stay inside these ranges and needn't reach their ends.
Inputs may be any that keep to these rules, and one draw needn't show every extreme that they name: `connectivity`: A number c of 256 or more names node c - 256 of the next node block; the last block's next block is the first. An element's eight corner numbers lie among min(8, 64) consecutive numbers; where these lie in the block is not tied to the element's position.
All inputs are finite; a program needn't handle non-finite values.
Results may differ from the reference program's by a relative error of at most 0.0072.
Values may be sent and summed in bfloat16 or wider, within the bound.
A program may use at most 64 MiB of HBM per device.

```python
import math
import jax
import jax.numpy as jnp
from jax import lax

MODES = 300
SNAP = 8
NODE_BLK = 256
GHOST = 64
NODES = 4096
ELEMS = 4096
N_ELEM = 16


def draw_modulus(key, part):
    position = jnp.arange(ELEMS, dtype=jnp.float32)
    rising = 1.0 + 2.0 * position / max(ELEMS - 1, 1)
    factor = jnp.exp(jax.random.uniform(key, (ELEMS,), jnp.float32, math.log(0.5), math.log(5.0)))
    return (rising * factor).astype(jnp.float32)


def draw_connectivity(key, part):
    window = min(8, GHOST)
    top_base = NODE_BLK + GHOST - window
    local_pos = jnp.arange(ELEMS, dtype=jnp.int32) % NODE_BLK
    random_base = jax.random.randint(jax.random.fold_in(key, 37), (ELEMS,), 0, top_base + 1, jnp.int32)
    base_node = jnp.where(local_pos == 0, 0, jnp.where(local_pos == NODE_BLK - 1, top_base, random_base)).astype(jnp.int32)
    scores = jax.random.randint(jax.random.fold_in(key, 31), (ELEMS, 8), 0, 1 << 20, jnp.int32)
    scores = scores * 8 + jnp.arange(8, dtype=jnp.int32)[None, :]
    ordering = jnp.argsort(scores, axis=1).astype(jnp.int32)
    offsets = ordering % window
    return (base_node[:, None] + offsets).astype(jnp.int32)


def draw_basis_rows(key, part):
    spacing = 8
    cells = -(-NODES // spacing)
    coarse = jax.random.normal(jax.random.fold_in(key, 41), (3, MODES, cells + 1), jnp.float32)
    fraction = (jnp.arange(spacing, dtype=jnp.float32) + 0.5) / spacing
    spread_norm = jnp.sqrt((1.0 - fraction) ** 2 + fraction ** 2)
    smooth = (coarse[:, :, :-1, None] * (1.0 - fraction) + coarse[:, :, 1:, None] * fraction) / spread_norm
    smooth = smooth.reshape(3, MODES, cells * spacing)[:, :, :NODES]
    node_pos = (jnp.arange(NODES, dtype=jnp.int32) % NODE_BLK).astype(jnp.float32) / NODE_BLK
    node_levels = jnp.exp(jax.random.uniform(jax.random.fold_in(key, 43), (NODES,), jnp.float32, math.log(0.7), math.log(1.4)))
    rough_part = jax.random.normal(jax.random.fold_in(key, 47), (3, MODES, NODES), jnp.float32)
    amplitude = (0.7 + 0.6 * node_pos) * node_levels
    shared = 0.35 + 0.55 * node_pos
    values = amplitude * (shared * smooth + jnp.sqrt(1.0 - shared * shared) * rough_part) / math.sqrt(MODES)
    return jnp.clip(values, -0.375, 0.375).astype(jnp.bfloat16)


def level_of(rng, extent, shards, smallest, high):
    level, own = 1.0, jax.random.fold_in(rng, 6)
    for axis_at, shards_of in shards:
        steps = jnp.exp(jax.random.uniform(jax.random.fold_in(own, axis_at), (shards_of,), jnp.float32, smallest / len(shards), high / len(shards)))
        level = level * jnp.repeat(steps, extent[axis_at] // shards_of).reshape([-1 if axis == axis_at else 1 for axis in range(len(extent))])
    return level


def scatter_about(key, extent, spread, reach, shards=(), held_as=jnp.bfloat16):
    loudness = level_of(key, extent, shards, -0.22, 0.18) if shards else 1.0
    values = jax.random.normal(key, extent, jnp.float32) * spread * loudness
    return jnp.minimum(jnp.maximum(values, -reach), reach).astype(held_as)


def setup_inputs(seed: int = 0) -> dict:
    key_of = jax.random.split(jax.random.key(seed), 6)
    coords = scatter_about(key_of[0], (SNAP, MODES), 1.0, 6.0, ((0, 2),))
    basis_rows = draw_basis_rows(jax.random.fold_in(key_of[5], 71), 0)
    connectivity = draw_connectivity(jax.random.fold_in(key_of[5], 71), 0)
    modulus = draw_modulus(jax.random.fold_in(key_of[5], 71), 0)
    stiffness = scatter_about(key_of[4], (24, 24), 24 ** -0.5, 1.25, (), jnp.float32)
    return {"coords": coords, "basis_rows": basis_rows, "connectivity": connectivity, "modulus": modulus, "stiffness": stiffness}


def block_columns(displaced, basis_rows, stiffness, corner_ids, mod_block):
    index_table = corner_ids.T
    count = index_table.shape[1]
    snaps = displaced.shape[0]
    corner_disp = displaced[:, :, index_table].reshape(snaps, 24, count).astype(jnp.float32)
    linear = jnp.einsum('kj,sje->ske', stiffness, corner_disp, precision=lax.Precision.HIGHEST)
    forces = (mod_block * (linear + 0.25 * corner_disp * corner_disp * corner_disp)).astype(jnp.bfloat16)
    forces = forces.reshape(snaps, 3, 8, count)
    element_basis = basis_rows[:, :, index_table]
    return jnp.einsum('cmae,scae->sme', element_basis.astype(jnp.float32), forces.astype(jnp.float32), precision=lax.Precision.HIGHEST)

def global_ids(block_id, conn_block):
    following = (block_id + 1) % N_ELEM
    return jnp.where(conn_block < NODE_BLK, block_id * NODE_BLK + conn_block, following * NODE_BLK + conn_block - NODE_BLK).astype(jnp.int32)

def reference(coords, basis_rows, connectivity, modulus, stiffness):
    displaced = jnp.stack([jnp.dot(coords, basis_rows[component], preferred_element_type=jnp.float32) for component in range(3)], axis=1).astype(jnp.bfloat16)
    conn_blocks = connectivity.reshape(N_ELEM, NODE_BLK, 8)
    mod_blocks = modulus.reshape(N_ELEM, NODE_BLK)
    block_ids = jnp.arange(N_ELEM, dtype=jnp.int32)

    def block_stats(inputs):
        block_id, conn_block, mod_block = inputs
        columns = block_columns(displaced, basis_rows, stiffness, global_ids(block_id, conn_block), mod_block)
        return (lax.optimization_barrier(jnp.sum(jnp.sqrt(lax.optimization_barrier(jnp.sum(columns * columns, axis=1))), axis=1)), lax.optimization_barrier(jnp.sum(columns, axis=2)))
    norm_parts, force_parts = lax.map(block_stats, (block_ids, conn_blocks, mod_blocks))
    row_scale = lax.optimization_barrier(jnp.sum(norm_parts, axis=0)) / ELEMS
    target = lax.optimization_barrier(jnp.sum(force_parts, axis=0)) / (row_scale[:, None] * math.sqrt(ELEMS))

    def block_output(inputs):
        block_id, conn_block, mod_block = inputs
        columns = block_columns(displaced, basis_rows, stiffness, global_ids(block_id, conn_block), mod_block)
        return (columns / row_scale[:, None, None]).astype(jnp.bfloat16)
    pieces = lax.map(block_output, (block_ids, conn_blocks, mod_blocks))
    training = jnp.transpose(pieces, (1, 2, 0, 3)).reshape(SNAP, MODES, ELEMS)
    return (training, target)
```

```python
import functools
import math

import jax
import jax.numpy as jnp
from jax import lax
from jax.experimental import pallas as pl
from jax.experimental.pallas import tpu as pltpu
from jax.sharding import PartitionSpec as P

MESH = pl.DeviceIdType.MESH
F32 = jnp.float32
BF16 = jnp.bfloat16
UNROLL = 64


def round_up(value, to):
    return -(-value // to) * to


def repeat(count, body):
    if count <= UNROLL:
        for j in range(count):
            body(j)
    else:
        lax.fori_loop(0, count, lambda j, c: (body(j), c)[1], 0)


def kernel(
    elems, params,
    coords_hbm, basis_hbm, conn_hbm, modulus_hbm, stiff_hbm,
    training_ref, target_ref,
    coords_ref, basis_ref, conn_ref, modulus_ref, stiff_ref,
    cols_ref, packed, ghost_in, ghost, disp, mask, weights, ghost_weights, acc, part,
    norms, part_p, part_e, total_ref,
    load, load_b, send_g, recv_g, send_d, recv_d, send_n, recv_n, send_f, recv_f,
    send_c, recv_c, send_p, recv_p, send_e, recv_e, send_t, recv_t,
):
    own_snaps, modes = coords_hbm.shape
    dofs = stiff_hbm.shape[0]
    snaps = own_snaps * params
    nodes = basis_hbm.shape[2]
    ghosts = nodes // 4
    total_nodes = nodes + ghosts
    count = conn_hbm.shape[1]
    devices = elems * params
    elem_total = count * devices
    me_e, me_p = lax.axis_index("elem"), lax.axis_index("param")
    me = me_e * params + me_p
    lead = params - 1
    before = (me_e + elems - 1) % elems

    def other(j):
        to = (me + j + 1) % devices
        return (to // params, to % params)

    barrier = pltpu.get_barrier_semaphore()
    repeat(devices - 1, lambda j: pl.semaphore_signal(
        barrier, inc=1, device_id=other(j), device_id_type=MESH))

    loads = [
        pltpu.make_async_copy(
            basis_hbm.at[k], basis_ref.at[:, pl.ds(k * nodes, nodes)], load_b.at[k]
        )
        for k in range(3)
    ]
    smalls = [
        pltpu.make_async_copy(src, dst, load.at[i])
        for i, (src, dst) in enumerate([
            (coords_hbm, coords_ref), (conn_hbm, conn_ref),
            (modulus_hbm, modulus_ref), (stiff_hbm, stiff_ref),
        ])
    ]
    for copy in smalls + loads:
        copy.start()

    def remote(src, dst, send, recv, device):
        return pltpu.make_async_remote_copy(
            src_ref=src, dst_ref=dst, send_sem=send, recv_sem=recv,
            device_id=device, device_id_type=MESH,
        )

    own_tiles = nodes // 128
    ghost_tiles = disp.shape[1] - own_tiles
    half = packed.shape[1]
    split = half < modes
    for copy in smalls:
        copy.wait()
    coords = coords_ref[...]
    for k in range(3):
        loads[k].wait()
        moved = jnp.dot(
            coords, basis_ref[:, k * nodes : (k + 1) * nodes], preferred_element_type=F32
        )
        moved = moved.astype(BF16).astype(F32)
        for t in range(own_tiles):
            disp[me_p, t, k] = moved[:, t * 128 : (t + 1) * 128]
    for k in range(3):
        at = k * nodes
        if split:
            packed[k, :, :ghosts] = basis_ref[:half, at : at + ghosts]
            packed[k, : modes - half, ghosts:] = basis_ref[half:, at : at + ghosts]
        else:
            packed[k, :modes] = basis_ref[:, at : at + ghosts]

    pl.semaphore_wait(barrier, devices - 1)
    own_part, ghost_part = pl.ds(0, own_tiles), pl.ds(own_tiles, ghost_tiles)
    sends, arrivals = [], []
    for p in range(params):
        turn = (me_p + p) % params
        source = (me_p + params - p) % params
        sends.append(remote(
            disp.at[me_p, pl.ds(0, ghost_tiles)], disp.at[me_p, ghost_part],
            send_d.at[p], recv_d.at[me_p], (before, turn),
        ))
        arrivals.append(remote(
            disp.at[source, pl.ds(0, ghost_tiles)], disp.at[source, ghost_part],
            send_d.at[p], recv_d.at[source], (before, turn),
        ))
        if p:
            sends.append(remote(
                disp.at[me_p, own_part], disp.at[me_p, own_part],
                send_n.at[p], recv_n.at[me_p], (me_e, turn),
            ))
            arrivals.append(remote(
                disp.at[source, own_part], disp.at[source, own_part],
                send_n.at[p], recv_n.at[source], (me_e, turn),
            ))
    for copy in sends:
        copy.start()
    ghost_copy = remote(packed, ghost_in, send_g, recv_g, (before, lead))
    hand_on = [
        remote(ghost_in, ghost_in, send_f.at[p], recv_f, (me_e, p)) for p in range(params - 1)
    ]

    @pl.when(me_p == lead)
    def _():
        ghost_copy.start()

    corners = conn_ref[...]
    base = jnp.min(corners, axis=0, keepdims=True)
    residue = corners % 8
    lane_at = corners % 128
    tile_at = corners // 128
    node = lax.broadcasted_iota(jnp.int32, (total_nodes, count), 0)
    inside = (node >= base) & (node < base + 8)
    mask[...] = jnp.where(inside, 1.0, 0.0).astype(BF16)
    stiff = stiff_ref[...]
    high = stiff.astype(BF16)
    rest = stiff - high.astype(F32)
    mid = rest.astype(BF16)
    low = (rest - mid.astype(F32)).astype(BF16)
    modulus = modulus_ref[...]
    modulus2 = jnp.concatenate([modulus, modulus], axis=1)
    part[...] = jnp.zeros_like(part)
    lane = lax.broadcasted_iota(jnp.int32, (1, 128), 1)
    row8 = lax.broadcasted_iota(jnp.int32, (8, count), 0)

    for copy in arrivals:
        copy.wait_recv()

    def own_product(p):
        pieces = []
        for at in range(2):
            s = 2 * p + at
            rows = []
            for k in range(3):
                found = jnp.zeros((8, count), F32)
                for t in range(disp.shape[1]):
                    line = disp[s // own_snaps, t, k, pl.ds(s % own_snaps, 1), :]
                    got = jnp.take_along_axis(jnp.broadcast_to(line, (8, 128)), lane_at, axis=1)
                    found = jnp.where(tile_at == t, got, found)
                rows.append(found)
            pieces.append(jnp.concatenate(rows, axis=0))
        moved = jnp.concatenate(pieces, axis=1)
        moved16 = moved.astype(BF16)
        linear = jnp.dot(low, moved16, preferred_element_type=F32)
        linear = linear + jnp.dot(mid, moved16, preferred_element_type=F32)
        linear = linear + jnp.dot(high, moved16, preferred_element_type=F32)
        forces = (modulus2 * (linear + 0.25 * moved * moved * moved)).astype(BF16).astype(F32)
        for at in range(2):
            for k in range(3):
                spread = jnp.zeros((8, count), F32)
                for a in range(8):
                    force = forces[k * 8 + a : k * 8 + a + 1, at * count : (at + 1) * count]
                    spread = spread + jnp.where(residue[a : a + 1] == row8, force, 0.0)
                twice = jnp.concatenate([spread, spread], axis=0).astype(BF16)
                tall = jnp.concatenate([twice] * (total_nodes // 16), axis=0) * mask[...]
                columns = slice(at * count, (at + 1) * count)
                weights[k * nodes : (k + 1) * nodes, columns] = tall[:nodes]
                ghost_weights[p, k * ghosts : (k + 1) * ghosts, columns] = tall[nodes:]
        acc[p] = jnp.dot(basis_ref[...], weights[...], preferred_element_type=F32)

    def whole_product(p, carry):
        sums, squares = carry
        result = acc[p] + jnp.dot(ghost[...], ghost_weights[p], preferred_element_type=F32)
        for at in range(2):
            s = 2 * p + at
            mine = result[:, at * count : (at + 1) * count]
            cols_ref[pl.ds(s, modes, stride=snaps), :] = mine
            norm = jnp.sum(mine * mine, axis=0, keepdims=True)
            squares = jnp.where(row == s, norm, squares)
            sums = jnp.where(lane == s, jnp.sum(mine, axis=1, keepdims=True), sums)
        return sums, squares

    pairs = snaps // 2
    if pairs <= 4:
        for p in range(pairs):
            own_product(p)
    else:
        lax.fori_loop(0, pairs, lambda p, c: (own_product(p), c)[1], 0)

    @pl.when(me_p == lead)
    def _():
        ghost_copy.wait_recv()
        for copy in hand_on:
            copy.start()

    @pl.when(me_p != lead)
    def _():
        remote(ghost_in, ghost_in, send_f.at[0], recv_f, (me_e, lead)).wait_recv()

    for k in range(3):
        if split:
            ghost[:half, k * ghosts : (k + 1) * ghosts] = ghost_in[k, :, :ghosts]
            ghost[half:, k * ghosts : (k + 1) * ghosts] = ghost_in[k, : modes - half, ghosts:]
        else:
            ghost[:, k * ghosts : (k + 1) * ghosts] = ghost_in[k, :modes]
    row = lax.broadcasted_iota(jnp.int32, (snaps, 128), 0)
    across = lax.broadcasted_iota(jnp.int32, (snaps, 128), 1)
    carry = (jnp.zeros((modes, 128), F32), jnp.zeros((snaps, count), F32))
    if pairs <= 4:
        for p in range(pairs):
            carry = whole_product(p, carry)
    else:
        carry = lax.fori_loop(0, pairs, whole_product, carry)
    sums, squares = carry

    norm = jnp.sum(jnp.sqrt(squares), axis=1, keepdims=True)
    norms[me] = jnp.sum(jnp.where(row == across, norm, 0.0), axis=0, keepdims=True)

    def norm_copy(j):
        return remote(norms.at[me], norms.at[me], send_c, recv_c, other(j))

    repeat(devices - 1, lambda j: norm_copy(j).start())

    wide = part_e.shape[2]
    part[:modes] = sums
    flat = jnp.concatenate(
        [jnp.transpose(part[t * 128 : (t + 1) * 128])[:snaps] for t in range(wide // 128)], axis=1
    )
    part_p[me_p] = flat

    def to_lead():
        return remote(part_p.at[me_p], part_p.at[me_p], send_p, recv_p.at[me_p], (me_e, lead))

    def to_elem(j):
        to = (me_e + j + 1) % elems
        return remote(part_e.at[me_e], part_e.at[me_e], send_e.at[j], recv_e.at[me_e], (to, lead))

    def from_elem(j):
        source = (me_e + elems - j - 1) % elems
        return remote(
            part_e.at[source], part_e.at[source], send_e.at[j], recv_e.at[source], (source, lead)
        )

    def result(p):
        return remote(total_ref, total_ref, send_t.at[p], recv_t, (me_e, p))

    @pl.when(me_p != lead)
    def _():
        to_lead().start()

    @pl.when(me_p == lead)
    def _():
        for p in range(params - 1):
            remote(part_p.at[p], part_p.at[p], send_p, recv_p.at[p], (me_e, p)).wait_recv()
        chip = part_p[0]
        for p in range(1, params):
            chip = chip + part_p[p]
        part_e[me_e] = chip
        repeat(elems - 1, lambda j: to_elem(j).start())

    everyone = norms.at[pl.ds(0, devices - 1)]
    gathered = pltpu.make_async_copy(everyone, everyone, recv_c)
    gathered.wait()
    whole = norms[0]
    for d in range(1, devices):
        whole = whole + norms[d]
    diagonal = jnp.where(row == across, jnp.broadcast_to(whole, (snaps, 128)), 0.0)
    row_scale = jnp.sum(diagonal, axis=1, keepdims=True) / elem_total
    inverse = jnp.broadcast_to(1.0 / row_scale, (snaps, count))
    piece = cols_ref[...].reshape(modes, snaps, count) * inverse[None]
    training_ref[...] = piece.astype(BF16)

    @pl.when(me_p == lead)
    def _():
        repeat(elems - 1, lambda j: from_elem(j).wait_recv())
        total = part_e[0]
        for e in range(1, elems):
            total = total + part_e[e]
        total_ref[...] = total
        for p in range(params - 1):
            result(p).start()

    @pl.when(me_p != lead)
    def _():
        remote(total_ref, total_ref, send_t.at[0], recv_t, (me_e, lead)).wait_recv()

    target_ref[...] = total_ref[:, :modes] / (row_scale * math.sqrt(elem_total))

    for copy in sends:
        copy.wait_send()
    pltpu.make_async_copy(everyone, everyone, send_c).wait()

    @pl.when(me_p == lead)
    def _():
        ghost_copy.wait_send()
        for copy in hand_on:
            copy.wait_send()
        repeat(elems - 1, lambda j: to_elem(j).wait_send())
        for p in range(params - 1):
            result(p).wait_send()

    @pl.when(me_p != lead)
    def _():
        to_lead().wait_send()


def finish_kernel(training_ref, target_ref, training_hbm, target_hbm, sem):
    copies = [
        pltpu.make_async_copy(target_ref, target_hbm, sem.at[0]),
        pltpu.make_async_copy(training_ref, training_hbm, sem.at[1]),
    ]
    for copy in copies:
        copy.start()
    for copy in copies:
        copy.wait()


def local(elems, params, coords, basis_rows, connectivity, modulus, stiffness):
    own_snaps, modes = coords.shape
    nodes = basis_rows.shape[2]
    count = connectivity.shape[0]
    snaps = own_snaps * params
    ghosts = nodes // 4
    half, across = (modes, ghosts) if ghosts % 128 == 0 else (round_up(-(-modes // 2), 32), 2 * ghosts)
    tiles = nodes // 128 + -(-ghosts // 128)
    wide = round_up(modes, 128)
    dofs = stiffness.shape[0]
    devices = elems * params
    dma = pltpu.SemaphoreType.DMA
    vmem = pl.BlockSpec(memory_space=pltpu.VMEM)
    hbm = pl.BlockSpec(memory_space=pltpu.HBM)
    training, target = pl.pallas_call(
        functools.partial(kernel, elems, params),
        out_shape=(
            jax.ShapeDtypeStruct((modes, snaps, count), BF16),
            jax.ShapeDtypeStruct((snaps, modes), F32),
        ),
        in_specs=[hbm] * 5,
        out_specs=(vmem, vmem),
        scratch_shapes=[
            pltpu.VMEM((own_snaps, modes), BF16),
            pltpu.VMEM((modes, 3 * nodes), BF16),
            pltpu.VMEM((8, count), jnp.int32),
            pltpu.VMEM((1, count), F32),
            pltpu.VMEM((dofs, dofs), F32),
            pltpu.VMEM((modes * snaps, count), F32),
            pltpu.VMEM((3, round_up(half, 16), across), BF16),
            pltpu.VMEM((3, round_up(half, 16), across), BF16),
            pltpu.VMEM((modes, 3 * ghosts), BF16),
            pltpu.VMEM((params, tiles, 3, own_snaps, 128), F32),
            pltpu.VMEM((nodes + ghosts, count), BF16),
            pltpu.VMEM((3 * nodes, 2 * count), BF16),
            pltpu.VMEM((snaps // 2, 3 * ghosts, 2 * count), BF16),
            pltpu.VMEM((snaps // 2, modes, 2 * count), F32),
            pltpu.VMEM((wide, 128), F32),
            pltpu.VMEM((devices, 1, 128), F32),
            pltpu.VMEM((params, snaps, wide), F32),
            pltpu.VMEM((elems, snaps, wide), F32),
            pltpu.VMEM((snaps, wide), F32),
            dma((4,)), dma((3,)), dma, dma,
            dma((params,)), dma((params,)),
            dma((params,)), dma((params,)),
            dma((params,)), dma,
            dma, dma,
            dma, dma((params,)),
            dma((elems,)), dma((elems,)),
            dma((params,)), dma,
        ],
        compiler_params=pltpu.CompilerParams(
            collective_id=0, has_side_effects=True, vmem_limit_bytes=40 * 1024 * 1024
        ),
    )(*(pltpu.with_memory_space_constraint(x, pltpu.HBM) for x in (
        coords, basis_rows, connectivity.T, modulus[None], stiffness
    )))
    training, target = pl.pallas_call(
        finish_kernel,
        out_shape=(
            jax.ShapeDtypeStruct((modes, snaps, count), BF16),
            jax.ShapeDtypeStruct((snaps, modes), F32),
        ),
        in_specs=[vmem, vmem],
        out_specs=(hbm, hbm),
        scratch_shapes=[dma((2,))],
        compiler_params=pltpu.CompilerParams(vmem_limit_bytes=20 * 1024 * 1024),
    )(training, target)
    return (jnp.transpose(training, (1, 0, 2)), target)


def solution(mesh):
    in_specs = (
        P("param", None),
        P(None, None, "elem"),
        P(("elem", "param"), None),
        P(("elem", "param")),
        P(),
    )
    out_specs = (P(None, None, ("elem", "param")), P())
    run = functools.partial(local, mesh.shape["elem"], mesh.shape["param"])
    return jax.shard_map(run, mesh=mesh, in_specs=in_specs, out_specs=out_specs, check_vma=False)
```

```python
import functools
import math

import jax
import jax.numpy as jnp
from jax import lax
from jax.experimental import pallas as pl
from jax.experimental.pallas import tpu as pltpu
from jax.sharding import PartitionSpec as P

LOGICAL = pl.DeviceIdType.LOGICAL
F32 = jnp.float32
BF16 = jnp.bfloat16
UNROLL = 64


def round_up(value, to):
    return -(-value // to) * to


def repeat(count, body):
    if count <= UNROLL:
        for j in range(count):
            body(j)
    else:
        lax.fori_loop(0, count, lambda j, c: (body(j), c)[1], 0)


def kernel(
    elems, params, inner,
    coords_hbm, basis_hbm, conn_hbm, modulus_hbm, stiff_hbm,
    training_ref, target_ref,
    coords_ref, basis_ref, conn_ref, modulus_ref, stiff_ref,
    cols_ref, packed, ghost_in, ghost, disp, mask, weights, ghost_weights, acc, part,
    norms, part_p, part_e, total_ref, relay_disp, relay_ghost,
    load, load_b, send_g, recv_g, send_d, recv_d, send_n, recv_n, send_f, recv_f,
    send_c, recv_c, send_p, recv_p, send_e, recv_e, send_t, recv_t,
    send_rd, recv_rd, send_rg, recv_rg, known,
):
    own_snaps, modes = coords_hbm.shape
    dofs = stiff_hbm.shape[0]
    snaps = own_snaps * params
    nodes = basis_hbm.shape[2]
    ghosts = nodes // 4
    total_nodes = nodes + ghosts
    count = conn_hbm.shape[1]
    devices = elems * params
    elem_total = count * devices
    me_e, me_p = lax.axis_index("elem"), lax.axis_index("param")
    me = me_e * params + me_p
    lead = params - 1
    first, last = me_e == 0, me_e == elems - 1
    before = jnp.where(first, elems - 1, me_e - 1)
    relay_e = elems // 4
    relay = relay_e * params + lead
    relaying = me == relay
    me_o = lax.div(me_e, inner)
    bottom, top = me_o == 0, me_o == elems // inner - 1

    def dev(e, p):
        return e * params + p

    def other(j):
        to = me + (j + 1)
        return jnp.where(to >= devices, to - devices, to)

    def flipped(index, stride):
        return jnp.where(lax.rem(lax.div(index, stride), 2) == 0, index + stride, index - stride)

    strides = [2**b for b in range(params.bit_length() - 1)]
    flips = [dev(me_e, flipped(me_p, stride)) for stride in strides]
    strides = [2**b for b in range(inner.bit_length() - 1)]
    flips += [dev(flipped(me_e, stride), me_p) for stride in strides]

    loads = [
        pltpu.make_async_copy(
            basis_hbm.at[k], basis_ref.at[:, pl.ds(k * nodes, nodes)], load_b.at[k]
        )
        for k in range(3)
    ]
    smalls = [
        pltpu.make_async_copy(src, dst, load.at[i])
        for i, (src, dst) in enumerate([
            (coords_hbm, coords_ref), (conn_hbm, conn_ref),
            (modulus_hbm, modulus_ref), (stiff_hbm, stiff_ref),
        ])
    ]
    for copy in loads + smalls:
        copy.start()

    barrier = pltpu.get_barrier_semaphore()

    def greet(device):
        pl.semaphore_signal(barrier, inc=1, device_id=device, device_id_type=LOGICAL)

    @pl.when(last | first)
    def _():
        greet(relay)

    @pl.when(relaying)
    def _():
        for p in range(params):
            greet(dev(elems - 1, p))
            greet(dev(0, p))

    @pl.when(jnp.logical_not(first))
    def _():
        for p in range(params):
            greet(dev(me_e - 1, p))

    @pl.when(jnp.logical_not(last))
    def _():
        for p in range(params):
            greet(dev(me_e + 1, p))

    @pl.when(jnp.logical_not(bottom))
    def _():
        greet(dev(me_e - inner, me_p))

    @pl.when(jnp.logical_not(top))
    def _():
        greet(dev(me_e + inner, me_p))

    for j in range(1, params):
        greet(dev(me_e, lax.rem(me_p + j, params)))
    for device in flips:
        greet(device)
    greeted = len(flips) + params - 1 + 2 * params + 2
    greeted += jnp.where(first | last, 1 - params, 0) + jnp.where(relaying, 2 * params, 0)
    greeted -= jnp.where(bottom | top, 1, 0)

    def remote(src, dst, send, recv, device):
        return pltpu.make_async_remote_copy(
            src_ref=src, dst_ref=dst, send_sem=send, recv_sem=recv,
            device_id=device, device_id_type=LOGICAL,
        )

    own_tiles = nodes // 128
    ghost_tiles = disp.shape[1] - own_tiles
    half = packed.shape[1]
    split = half < modes
    for copy in smalls:
        copy.wait()
    coords = coords_ref[...]
    for k in range(3):
        loads[k].wait()
        moved = jnp.dot(
            coords, basis_ref[:, k * nodes : (k + 1) * nodes], preferred_element_type=F32
        )
        moved = moved.astype(BF16).astype(F32)
        for t in range(own_tiles):
            disp[me_p, t, k] = moved[:, t * 128 : (t + 1) * 128]
    for k in range(3):
        at = k * nodes
        if split:
            packed[k, :, :ghosts] = basis_ref[:half, at : at + ghosts]
            packed[k, : modes - half, ghosts:] = basis_ref[half:, at : at + ghosts]
        else:
            packed[k, :modes] = basis_ref[:, at : at + ghosts]

    pl.semaphore_wait(barrier, greeted)
    own_part, ghost_part = pl.ds(0, own_tiles), pl.ds(own_tiles, ghost_tiles)
    front = disp.at[me_p, pl.ds(0, ghost_tiles)]
    back = [disp.at[p, ghost_part] for p in range(params)]
    mine_back = disp.at[me_p, ghost_part]

    def ghost_disp(p):
        turn = lax.rem(me_p + p, params)
        return remote(front, mine_back, send_d.at[p], recv_d.at[me_p], dev(before, turn))

    def own_disp(p):
        turn = lax.rem(me_p + p, params)
        mine = disp.at[me_p, own_part]
        return remote(mine, mine, send_n.at[p], recv_n.at[me_p], dev(me_e, turn))

    def to_relay():
        return remote(front, relay_disp.at[me_p], send_d.at[0], recv_rd.at[me_p], relay)

    def from_relay(q, p):
        return remote(
            relay_disp.at[q], back[q], send_rd.at[q * params + p], recv_d.at[q], dev(elems - 1, p)
        )

    def ghost_copy():
        return remote(packed, ghost_in, send_g, recv_g, dev(before, lead))

    def ghost_to_relay():
        return remote(packed, relay_ghost, send_g, recv_rg, relay)

    def ghost_from_relay():
        return remote(relay_ghost, ghost_in, send_rg, recv_g, dev(elems - 1, lead))

    def hand_on(p):
        return remote(ghost_in, ghost_in, send_f.at[p], recv_f, dev(me_e, p))

    @pl.when(first)
    def _():
        to_relay().start()

    @pl.when(jnp.logical_not(first))
    def _():
        for p in range(params):
            ghost_disp(p).start()

    @pl.when(first & (me_p == lead))
    def _():
        ghost_to_relay().start()

    @pl.when(jnp.logical_not(first) & (me_p == lead))
    def _():
        ghost_copy().start()

    for p in range(1, params):
        own_disp(p).start()

    @pl.when(relaying)
    def _():
        for q in range(params):
            remote(front, relay_disp.at[q], send_d.at[0], recv_rd.at[q], relay).wait_recv()
        for q in range(params):
            for p in range(params):
                from_relay(q, params - 1 - p).start()
        ghost_to_relay().wait_recv()
        ghost_from_relay().start()

    corners = conn_ref[...]
    base = jnp.min(corners, axis=0, keepdims=True)
    residue = corners % 8
    lane_at = corners % 128
    tile_at = corners // 128
    node = lax.broadcasted_iota(jnp.int32, (total_nodes, count), 0)
    inside = (node >= base) & (node < base + 8)
    mask[...] = jnp.where(inside, 1.0, 0.0).astype(BF16)
    stiff = stiff_ref[...]
    high = stiff.astype(BF16)
    rest = stiff - high.astype(F32)
    mid = rest.astype(BF16)
    low = (rest - mid.astype(F32)).astype(BF16)
    modulus = modulus_ref[...]
    modulus2 = jnp.concatenate([modulus, modulus], axis=1)
    part[...] = jnp.zeros_like(part)
    lane = lax.broadcasted_iota(jnp.int32, (1, 128), 1)
    row8 = lax.broadcasted_iota(jnp.int32, (8, count), 0)

    def tell(at, device):
        pl.semaphore_signal(known.at[at], inc=1, device_id=device, device_id_type=LOGICAL)

    for at, device in enumerate(flips):
        tell(at, device)
        pl.semaphore_wait(known.at[at], 1)
    up, down = len(flips), len(flips) + 1

    @pl.when(jnp.logical_not(bottom))
    def _():
        pl.semaphore_wait(known.at[up], 1)

    @pl.when(jnp.logical_not(top))
    def _():
        tell(up, dev(me_e + inner, me_p))
        pl.semaphore_wait(known.at[down], 1)

    @pl.when(jnp.logical_not(bottom))
    def _():
        tell(down, dev(me_e - inner, me_p))

    for q in range(params):
        remote(front, back[q], send_d.at[0], recv_d.at[q], me).wait_recv()
    for j in range(1, params):
        q = lax.rem(me_p + j, params)
        own = disp.at[q, own_part]
        remote(own, own, send_n.at[0], recv_n.at[q], me).wait_recv()

    def own_product(p):
        pieces = []
        for at in range(2):
            s = 2 * p + at
            rows = []
            for k in range(3):
                found = jnp.zeros((8, count), F32)
                for t in range(disp.shape[1]):
                    line = disp[s // own_snaps, t, k, pl.ds(s % own_snaps, 1), :]
                    got = jnp.take_along_axis(jnp.broadcast_to(line, (8, 128)), lane_at, axis=1)
                    found = jnp.where(tile_at == t, got, found)
                rows.append(found)
            pieces.append(jnp.concatenate(rows, axis=0))
        moved = jnp.concatenate(pieces, axis=1)
        moved16 = moved.astype(BF16)
        linear = jnp.dot(low, moved16, preferred_element_type=F32)
        linear = linear + jnp.dot(mid, moved16, preferred_element_type=F32)
        linear = linear + jnp.dot(high, moved16, preferred_element_type=F32)
        forces = (modulus2 * (linear + 0.25 * moved * moved * moved)).astype(BF16).astype(F32)
        for at in range(2):
            for k in range(3):
                spread = jnp.zeros((8, count), F32)
                for a in range(8):
                    force = forces[k * 8 + a : k * 8 + a + 1, at * count : (at + 1) * count]
                    spread = spread + jnp.where(residue[a : a + 1] == row8, force, 0.0)
                twice = jnp.concatenate([spread, spread], axis=0).astype(BF16)
                tall = jnp.concatenate([twice] * (total_nodes // 16), axis=0) * mask[...]
                columns = slice(at * count, (at + 1) * count)
                weights[k * nodes : (k + 1) * nodes, columns] = tall[:nodes]
                ghost_weights[p, k * ghosts : (k + 1) * ghosts, columns] = tall[nodes:]
        acc[p] = jnp.dot(basis_ref[...], weights[...], preferred_element_type=F32)

    def whole_product(p, carry):
        sums, squares = carry
        result = acc[p] + jnp.dot(ghost[...], ghost_weights[p], preferred_element_type=F32)
        for at in range(2):
            s = 2 * p + at
            mine = result[:, at * count : (at + 1) * count]
            cols_ref[pl.ds(s, modes, stride=snaps), :] = mine
            norm = jnp.sum(mine * mine, axis=0, keepdims=True)
            squares = jnp.where(row == s, norm, squares)
            sums = jnp.where(lane == s, jnp.sum(mine, axis=1, keepdims=True), sums)
        return sums, squares

    pairs = snaps // 2
    if pairs <= 4:
        for p in range(pairs):
            own_product(p)
    else:
        lax.fori_loop(0, pairs, lambda p, c: (own_product(p), c)[1], 0)

    @pl.when(me_p == lead)
    def _():
        ghost_copy().wait_recv()
        for p in range(params - 1):
            hand_on(p).start()

    @pl.when(me_p != lead)
    def _():
        hand_on(0).wait_recv()

    for k in range(3):
        if split:
            ghost[:half, k * ghosts : (k + 1) * ghosts] = ghost_in[k, :, :ghosts]
            ghost[half:, k * ghosts : (k + 1) * ghosts] = ghost_in[k, : modes - half, ghosts:]
        else:
            ghost[:, k * ghosts : (k + 1) * ghosts] = ghost_in[k, :modes]
    row = lax.broadcasted_iota(jnp.int32, (snaps, 128), 0)
    across = lax.broadcasted_iota(jnp.int32, (snaps, 128), 1)
    carry = (jnp.zeros((modes, 128), F32), jnp.zeros((snaps, count), F32))
    if pairs <= 4:
        for p in range(pairs):
            carry = whole_product(p, carry)
    else:
        carry = lax.fori_loop(0, pairs, whole_product, carry)
    sums, squares = carry

    norm = jnp.sum(jnp.sqrt(squares), axis=1, keepdims=True)
    norms[me] = jnp.sum(jnp.where(row == across, norm, 0.0), axis=0, keepdims=True)

    def norm_copy(j):
        return remote(norms.at[me], norms.at[me], send_c, recv_c, other(j))

    repeat(devices - 1, lambda j: norm_copy(j).start())

    wide = part_e.shape[2]
    part[:modes] = sums
    flat = jnp.concatenate(
        [jnp.transpose(part[t * 128 : (t + 1) * 128])[:snaps] for t in range(wide // 128)], axis=1
    )
    part_p[me_p] = flat

    def to_lead():
        return remote(part_p.at[me_p], part_p.at[me_p], send_p, recv_p.at[me_p], dev(me_e, lead))

    def wrapped(e):
        return jnp.where(e >= elems, e - elems, e)

    def to_elem(j):
        to = wrapped(me_e + (j + 1))
        return remote(part_e.at[me_e], part_e.at[me_e], send_e.at[j], recv_e.at[me_e], dev(to, lead))

    def from_elem(j):
        source = wrapped(me_e + elems - j - 1)
        return remote(
            part_e.at[source], part_e.at[source], send_e.at[j], recv_e.at[source], dev(source, lead)
        )

    def result(p):
        return remote(total_ref, total_ref, send_t.at[p], recv_t, dev(me_e, p))

    @pl.when(me_p != lead)
    def _():
        to_lead().start()

    @pl.when(me_p == lead)
    def _():
        for p in range(params - 1):
            remote(part_p.at[p], part_p.at[p], send_p, recv_p.at[p], me).wait_recv()
        chip = part_p[0]
        for p in range(1, params):
            chip = chip + part_p[p]
        part_e[me_e] = chip
        repeat(elems - 1, lambda j: to_elem(j).start())

    everyone = norms.at[pl.ds(0, devices - 1)]
    gathered = pltpu.make_async_copy(everyone, everyone, recv_c)
    gathered.wait()
    whole = norms[0]
    for d in range(1, devices):
        whole = whole + norms[d]
    diagonal = jnp.where(row == across, jnp.broadcast_to(whole, (snaps, 128)), 0.0)
    row_scale = jnp.sum(diagonal, axis=1, keepdims=True) / elem_total
    inverse = jnp.broadcast_to(1.0 / row_scale, (snaps, count))
    piece = cols_ref[...].reshape(modes, snaps, count) * inverse[None]
    training_ref[...] = piece.astype(BF16)

    @pl.when(me_p == lead)
    def _():
        repeat(elems - 1, lambda j: from_elem(j).wait_recv())
        total = part_e[0]
        for e in range(1, elems):
            total = total + part_e[e]
        total_ref[...] = total
        for p in range(params - 1):
            result(p).start()

    @pl.when(me_p != lead)
    def _():
        result(0).wait_recv()

    target_ref[...] = total_ref[:, :modes] / (row_scale * math.sqrt(elem_total))

    for p in range(1, params):
        own_disp(p).wait_send()
    pltpu.make_async_copy(everyone, everyone, send_c).wait()

    @pl.when(first)
    def _():
        to_relay().wait_send()

    @pl.when(jnp.logical_not(first))
    def _():
        for p in range(params):
            ghost_disp(p).wait_send()

    @pl.when(relaying)
    def _():
        for q in range(params):
            for p in range(params):
                from_relay(q, p).wait_send()
        ghost_from_relay().wait_send()

    @pl.when(me_p == lead)
    def _():
        ghost_copy().wait_send()
        for p in range(params - 1):
            hand_on(p).wait_send()
        repeat(elems - 1, lambda j: to_elem(j).wait_send())
        for p in range(params - 1):
            result(p).wait_send()

    @pl.when(me_p != lead)
    def _():
        to_lead().wait_send()


def finish_kernel(training_ref, target_ref, training_hbm, target_hbm, sem):
    copies = [
        pltpu.make_async_copy(target_ref, target_hbm, sem.at[0]),
        pltpu.make_async_copy(training_ref, training_hbm, sem.at[1]),
    ]
    for copy in copies:
        copy.start()
    for copy in copies:
        copy.wait()


def local(elems, params, coords, basis_rows, connectivity, modulus, stiffness):
    own_snaps, modes = coords.shape
    nodes = basis_rows.shape[2]
    count = connectivity.shape[0]
    snaps = own_snaps * params
    ghosts = nodes // 4
    half, across = (modes, ghosts) if ghosts % 128 == 0 else (round_up(-(-modes // 2), 32), 2 * ghosts)
    tiles = nodes // 128 + -(-ghosts // 128)
    wide = round_up(modes, 128)
    dofs = stiffness.shape[0]
    devices = elems * params
    inner = 4
    rounds = params.bit_length() + inner.bit_length() - 2
    dma = pltpu.SemaphoreType.DMA
    vmem = pl.BlockSpec(memory_space=pltpu.VMEM)
    hbm = pl.BlockSpec(memory_space=pltpu.HBM)
    training, target = pl.pallas_call(
        functools.partial(kernel, elems, params, inner),
        out_shape=(
            jax.ShapeDtypeStruct((modes, snaps, count), BF16),
            jax.ShapeDtypeStruct((snaps, modes), F32),
        ),
        in_specs=[hbm] * 5,
        out_specs=(vmem, vmem),
        scratch_shapes=[
            pltpu.VMEM((own_snaps, modes), BF16),
            pltpu.VMEM((modes, 3 * nodes), BF16),
            pltpu.VMEM((8, count), jnp.int32),
            pltpu.VMEM((1, count), F32),
            pltpu.VMEM((dofs, dofs), F32),
            pltpu.VMEM((modes * snaps, count), F32),
            pltpu.VMEM((3, round_up(half, 16), across), BF16),
            pltpu.VMEM((3, round_up(half, 16), across), BF16),
            pltpu.VMEM((modes, 3 * ghosts), BF16),
            pltpu.VMEM((params, tiles, 3, own_snaps, 128), F32),
            pltpu.VMEM((nodes + ghosts, count), BF16),
            pltpu.VMEM((3 * nodes, 2 * count), BF16),
            pltpu.VMEM((snaps // 2, 3 * ghosts, 2 * count), BF16),
            pltpu.VMEM((snaps // 2, modes, 2 * count), F32),
            pltpu.VMEM((wide, 128), F32),
            pltpu.VMEM((devices, 1, 128), F32),
            pltpu.VMEM((params, snaps, wide), F32),
            pltpu.VMEM((elems, snaps, wide), F32),
            pltpu.VMEM((snaps, wide), F32),
            pltpu.VMEM((params, tiles - nodes // 128, 3, own_snaps, 128), F32),
            pltpu.VMEM((3, round_up(half, 16), across), BF16),
            dma((4,)), dma((3,)), dma, dma,
            dma((params,)), dma((params,)),
            dma((params,)), dma((params,)),
            dma((params,)), dma,
            dma, dma,
            dma, dma((params,)),
            dma((elems,)), dma((elems,)),
            dma((params,)), dma,
            dma((params * params,)), dma((params,)), dma, dma,
            pltpu.SemaphoreType.REGULAR((rounds + 2,)),
        ],
        compiler_params=pltpu.CompilerParams(
            collective_id=0, has_side_effects=True, vmem_limit_bytes=40 * 1024 * 1024
        ),
    )(*(pltpu.with_memory_space_constraint(x, pltpu.HBM) for x in (
        coords, basis_rows, connectivity.T, modulus[None], stiffness
    )))
    training, target = pl.pallas_call(
        finish_kernel,
        out_shape=(
            jax.ShapeDtypeStruct((modes, snaps, count), BF16),
            jax.ShapeDtypeStruct((snaps, modes), F32),
        ),
        in_specs=[vmem, vmem],
        out_specs=(hbm, hbm),
        scratch_shapes=[dma((2,))],
        compiler_params=pltpu.CompilerParams(vmem_limit_bytes=20 * 1024 * 1024),
    )(training, target)
    return (jnp.transpose(training, (1, 0, 2)), target)


def solution(mesh):
    in_specs = (
        P("param", None),
        P(None, None, "elem"),
        P(("elem", "param"), None),
        P(("elem", "param")),
        P(),
    )
    out_specs = (P(None, None, ("elem", "param")), P())
    run = functools.partial(local, mesh.shape["elem"], mesh.shape["param"])
    return jax.shard_map(run, mesh=mesh, in_specs=in_specs, out_specs=out_specs, check_vma=False)
```

```python
import functools
import math

import jax
import jax.numpy as jnp
from jax import lax
from jax.experimental import pallas as pl
from jax.experimental.pallas import tpu as pltpu
from jax.sharding import PartitionSpec as P

LOGICAL = pl.DeviceIdType.LOGICAL
F32 = jnp.float32
BF16 = jnp.bfloat16
UNROLL = 64


def round_up(value, to):
    return -(-value // to) * to


def repeat(count, body):
    if count <= UNROLL:
        for j in range(count):
            body(j)
    else:
        lax.fori_loop(0, count, lambda j, c: (body(j), c)[1], 0)


def kernel(
    elems, params, inner,
    coords_hbm, basis_hbm, conn_hbm, modulus_hbm, stiff_hbm,
    training_ref, target_ref,
    coords_ref, basis_ref, conn_ref, modulus_ref, stiff_ref,
    packed, ghost_in, ghost, disp, corner_disp, weights, edge_weights, acc, cols_ref, part, nodal,
    norms, part_p, part_e, total_ref, relay_disp, relay_ghost,
    load, load_b, send_g, recv_g, send_d, recv_d, send_n, recv_n, send_f, recv_f,
    send_c, recv_c, send_p, recv_p, send_e, recv_e, send_t, recv_t,
    send_rd, recv_rd, send_rg, recv_rg, climb, known,
):
    own_snaps, modes = coords_hbm.shape
    dofs = stiff_hbm.shape[0]
    snaps = own_snaps * params
    pairs = snaps // 2
    nodes = basis_hbm.shape[2]
    ghosts = nodes // 4
    count = conn_hbm.shape[1]
    devices = elems * params
    outer = elems // inner
    elem_total = count * devices
    wide, edge = part_e.shape[2], ghost.shape[1]
    own_tiles = nodes // 128
    ghost_tiles = disp.shape[1] - own_tiles
    me_e, me_p = lax.axis_index("elem"), lax.axis_index("param")
    me = me_e * params + me_p
    lead = params - 1
    leading = me_p == lead
    first, last = me_e == 0, me_e == elems - 1
    before = jnp.where(first, elems - 1, me_e - 1)
    relay = elems // 4 * params + lead
    relaying = me == relay
    me_o, me_i = lax.div(me_e, inner), lax.rem(me_e, inner)
    bottom, top = me_o == 0, me_o == outer - 1
    climbing = me_p == 0

    def dev(e, p):
        return e * params + p

    def other(j):
        to = me + (j + 1)
        return jnp.where(to >= devices, to - devices, to)

    def signal(semaphore, device):
        pl.semaphore_signal(semaphore, inc=1, device_id=device, device_id_type=LOGICAL)

    def remote(src, dst, send, recv, device):
        return pltpu.make_async_remote_copy(
            src_ref=src, dst_ref=dst, send_sem=send, recv_sem=recv,
            device_id=device, device_id_type=LOGICAL,
        )

    def wait_bytes(ref, semaphore):
        pltpu.make_async_copy(ref, ref, semaphore).wait()

    load_basis = pltpu.make_async_copy(basis_hbm, basis_ref, load_b)
    smalls = [
        pltpu.make_async_copy(src, dst, load.at[i])
        for i, (src, dst) in enumerate([
            (coords_hbm, coords_ref), (conn_hbm, conn_ref),
            (modulus_hbm, modulus_ref), (stiff_hbm, stiff_ref),
        ])
    ]
    for copy in [load_basis] + smalls:
        copy.start()

    barrier = pltpu.get_barrier_semaphore()
    below = jnp.logical_not(first) & (me_i == 0)
    above = jnp.logical_not(last) & (me_i == inner - 1)

    @pl.when(first | last)
    def _():
        signal(barrier, relay)

    @pl.when(relaying)
    def _():
        for p in range(params):
            signal(barrier, dev(elems - 1, p))
            signal(barrier, dev(0, p))

    @pl.when(below)
    def _():
        for p in range(params):
            signal(barrier, dev(me_e - 1, p))

    @pl.when(above)
    def _():
        for p in range(params):
            signal(barrier, dev(me_e + 1, p))

    @pl.when(climbing & jnp.logical_not(bottom))
    def _():
        signal(barrier, dev(me_e - inner, 0))

    @pl.when(climbing & jnp.logical_not(top))
    def _():
        signal(barrier, dev(me_e + inner, 0))

    plane = inner * params
    place = me_i * params + me_p
    for j in range(1, plane):
        to = place + j
        signal(barrier, me_o * plane + jnp.where(to >= plane, to - plane, to))
    greeted = plane - 1 + jnp.where(first | last, 1, 0) + jnp.where(relaying, 2 * params, 0)
    greeted += jnp.where(below, params, 0) + jnp.where(above, params, 0)
    greeted += jnp.where(climbing & jnp.logical_not(bottom), 1, 0)
    greeted += jnp.where(climbing & jnp.logical_not(top), 1, 0)

    part[...] = jnp.zeros_like(part)
    nodal[...] = jnp.zeros_like(nodal)
    tail_at = 3 * ghosts
    for p in range(pairs):
        edge_weights[p, tail_at:] = jnp.zeros((edge - tail_at, 2 * count), BF16)
    for copy in smalls:
        copy.wait()
    coords = coords_ref[...]
    load_basis.wait()
    for k in range(3):
        moved = jnp.dot(coords, basis_ref[k], preferred_element_type=F32)
        moved = moved.astype(BF16).astype(F32)
        for t in range(own_tiles):
            disp[me_p, t, k] = moved[:, t * 128 : (t + 1) * 128]
    rows = packed.shape[0]
    if ghosts % 128 == 0:
        for k in range(3):
            packed[:modes, k * ghosts : (k + 1) * ghosts] = basis_ref[k, :, :ghosts]
    else:
        half = rows - round_up(modes, 16)
        packed[:modes, :ghosts] = basis_ref[0, :, :ghosts]
        packed[:modes, ghosts:] = basis_ref[1, :, :ghosts]
        packed[rows - half :, :ghosts] = basis_ref[2, :half, :ghosts]
        packed[rows - half : rows - 2 * half + modes, ghosts:] = basis_ref[2, half:, :ghosts]

    pl.semaphore_wait(barrier, greeted)
    own_part, ghost_part = pl.ds(0, own_tiles), pl.ds(own_tiles, ghost_tiles)
    front = disp.at[me_p, pl.ds(0, ghost_tiles)]
    backs = disp.at[:, ghost_part]

    def ghost_disp(p):
        turn = lax.rem(me_p + p, params)
        return remote(front, disp.at[me_p, ghost_part], send_d, recv_d, dev(before, turn))

    def own_disp(p):
        turn = lax.rem(me_p + p, params)
        mine = disp.at[me_p, own_part]
        return remote(mine, mine, send_n, recv_n, dev(me_e, turn))

    def to_relay():
        return remote(front, relay_disp.at[me_p], send_d, recv_rd, relay)

    def from_relay(q, p):
        return remote(
            relay_disp.at[q], disp.at[q, ghost_part], send_rd.at[q], recv_d, dev(elems - 1, p)
        )

    def ghost_copy():
        return remote(packed, ghost_in, send_g, recv_g, dev(before, lead))

    def ghost_to_relay():
        return remote(packed, relay_ghost, send_g, recv_rg, relay)

    def ghost_from_relay():
        return remote(relay_ghost, ghost_in, send_rg, recv_g, dev(elems - 1, lead))

    def hand_on(p):
        return remote(ghost_in, ghost_in, send_f.at[p], recv_f, dev(me_e, p))

    @pl.when(first)
    def _():
        to_relay().start()

    @pl.when(jnp.logical_not(first))
    def _():
        for p in range(params):
            ghost_disp(p).start()

    @pl.when(first & leading)
    def _():
        ghost_to_relay().start()

    @pl.when(jnp.logical_not(first) & leading)
    def _():
        ghost_copy().start()

    for p in range(1, params):
        own_disp(p).start()

    @pl.when(relaying)
    def _():
        wait_bytes(relay_disp, recv_rd)
        for q in range(params):
            for p in range(params):
                from_relay(q, params - 1 - p).start()
        ghost_to_relay().wait_recv()
        ghost_from_relay().start()

    @pl.when(climbing & jnp.logical_not(bottom))
    def _():
        pl.semaphore_wait(climb, 1)

    @pl.when(climbing & jnp.logical_not(top))
    def _():
        signal(climb, dev(me_e + inner, 0))

    @pl.when(climbing & top)
    def _():
        for p in range(1, params):
            signal(known, dev(me_e, p))
        for o in range(outer - 1):
            for p in range(params):
                signal(known, dev(o * inner + me_i, p))

    corners = conn_ref[...]
    base = jnp.min(corners, axis=0, keepdims=True)
    residue = corners % 8
    lane_at = corners % 128
    tile_at = corners // 128
    row8 = lax.broadcasted_iota(jnp.int32, (8, count), 0)
    lane = lax.broadcasted_iota(jnp.int32, (1, 128), 1)
    hits = [residue[a : a + 1] == row8 for a in range(8)]

    def inside(start, height):
        node = start + lax.broadcasted_iota(jnp.int32, (height, count), 0)
        return (node >= base) & (node < base + 8)

    own_rows = lax.broadcasted_iota(jnp.int32, (nodes, count), 0) < nodes - 8
    own_mask = jnp.where(inside(0, nodes) & own_rows, 1.0, 0.0).astype(BF16)
    ghost_mask = jnp.where(inside(nodes, ghosts), 1.0, 0.0)
    tail_mask = jnp.where(inside(nodes - 8, 8), 1.0, 0.0)
    stiff = stiff_ref[...]
    high = stiff.astype(BF16)
    rest = stiff - high.astype(F32)
    mid = rest.astype(BF16)
    low = (rest - mid.astype(F32)).astype(BF16)
    modulus = modulus_ref[...]
    modulus2 = jnp.concatenate([modulus, modulus], axis=1)
    tails = [basis_ref[k, :, nodes - 8 :] for k in range(3)]
    start = tail_at // 128 * 128
    blank = [jnp.zeros((modes, tail_at - start), BF16)] if tail_at > start else []
    after = [jnp.zeros((modes, edge - tail_at - 24), BF16)]
    ghost[:, start:] = jnp.concatenate(blank + tails + after, axis=1)

    def gathered(p, found, tiles):
        pieces = []
        for at in range(2):
            s = 2 * p + at
            parts = []
            for k in range(3):
                piece = found[k * 8 : (k + 1) * 8, at * count : (at + 1) * count]
                for t in tiles:
                    line = disp[s // own_snaps, t, k, pl.ds(s % own_snaps, 1), :]
                    got = jnp.take_along_axis(jnp.broadcast_to(line, (8, 128)), lane_at, axis=1)
                    piece = jnp.where(tile_at == t, got, piece)
                parts.append(piece)
            pieces.append(jnp.concatenate(parts, axis=0))
        return jnp.concatenate(pieces, axis=1)

    def forces_of(moved):
        moved16 = moved.astype(BF16)
        linear = jnp.dot(low, moved16, preferred_element_type=F32)
        linear = linear + jnp.dot(mid, moved16, preferred_element_type=F32)
        linear = linear + jnp.dot(high, moved16, preferred_element_type=F32)
        return (modulus2 * (linear + 0.25 * moved * moved * moved)).astype(BF16).astype(F32)

    def spread_of(forces, at, k):
        spread = jnp.zeros((8, count), F32)
        for a in range(8):
            force = forces[k * 8 + a : k * 8 + a + 1, at * count : (at + 1) * count]
            spread = spread + jnp.where(hits[a], force, 0.0)
        return spread.astype(BF16).astype(F32)

    def own_product(p):
        slot = p if weights.shape[0] > 1 else 0
        moved = gathered(p, jnp.zeros((dofs, 2 * count), F32), range(own_tiles))
        corner_disp[p] = moved
        forces = forces_of(moved)
        for at in range(2):
            columns = slice(at * count, (at + 1) * count)
            for k in range(3):
                spread = spread_of(forces, at, k)
                twice = jnp.concatenate([spread, spread], axis=0).astype(BF16)
                tall = jnp.concatenate([twice] * (nodes // 16), axis=0) * own_mask
                weights[slot, k * nodes : (k + 1) * nodes, columns] = tall
        total = jnp.dot(basis_ref[0], weights[slot, :nodes], preferred_element_type=F32)
        for k in range(1, 3):
            total = total + jnp.dot(
                basis_ref[k], weights[slot, k * nodes : (k + 1) * nodes], preferred_element_type=F32
            )
        acc[p] = total

    def own_sums(p):
        for at in range(2):
            mine = acc[p, :, at * count : (at + 1) * count]
            total = jnp.sum(mine, axis=1, keepdims=True)
            part[:modes] = jnp.where(lane == 2 * p + at, total, part[:modes])

    def edge_forces(p):
        moved = gathered(p, corner_disp[p], range(own_tiles, own_tiles + ghost_tiles))
        forces = forces_of(moved)
        for at in range(2):
            columns = slice(at * count, (at + 1) * count)
            ends = []
            for k in range(3):
                spread = spread_of(forces, at, k)
                tall = jnp.concatenate([spread] * (ghosts // 8), axis=0) * ghost_mask
                edge_weights[p, k * ghosts : (k + 1) * ghosts, columns] = tall.astype(BF16)
                ends.append(spread * tail_mask)
                total = jnp.sum(tall, axis=1, keepdims=True)
                at_rows = slice(k * ghosts, (k + 1) * ghosts)
                nodal[at_rows] = jnp.where(lane == 2 * p + at, total, nodal[at_rows])
            end = jnp.concatenate(ends + [jnp.zeros((8, count), F32)], axis=0)
            edge_weights[p, tail_at : tail_at + 32, columns] = end.astype(BF16)
            total = jnp.sum(end, axis=1, keepdims=True)
            at_rows = slice(tail_at, tail_at + 32)
            nodal[at_rows] = jnp.where(lane == 2 * p + at, total, nodal[at_rows])

    def whole_product(p, squares):
        result = acc[p] + jnp.dot(ghost[...], edge_weights[p], preferred_element_type=F32)
        for at in range(2):
            s = 2 * p + at
            mine = result[:, at * count : (at + 1) * count]
            cols_ref[pl.ds(s, modes, stride=snaps), :] = mine
            norm = jnp.sum(mine * mine, axis=0, keepdims=True)
            squares = jnp.where(row == s, norm, squares)
        return squares

    def each_pair(body):
        if pairs <= 4:
            for p in range(pairs):
                body(p)
        else:
            lax.fori_loop(0, pairs, lambda p, c: (body(p), c)[1], 0)

    others = disp.at[pl.ds(0, params - 1), own_part]
    wait_bytes(others, recv_n)
    each_pair(own_product)
    each_pair(own_sums)

    def flipped(ref):
        return jnp.concatenate(
            [jnp.transpose(ref[t * 128 : (t + 1) * 128])[:snaps] for t in range(ref.shape[0] // 128)],
            axis=1,
        )

    part_p[me_p, :, :wide] = flipped(part)
    wait_bytes(backs, recv_d)
    each_pair(edge_forces)
    part_p[me_p, :, wide:] = flipped(nodal)

    def to_lead():
        return remote(part_p.at[me_p], part_p.at[me_p], send_p, recv_p, dev(me_e, lead))

    @pl.when(jnp.logical_not(leading))
    def _():
        to_lead().start()

    @pl.when(leading)
    def _():
        ghost_copy().wait_recv()
        for p in range(params - 1):
            hand_on(p).start()

    @pl.when(jnp.logical_not(leading))
    def _():
        hand_on(0).wait_recv()

    if ghosts % 128 == 0:
        ghost[:, :tail_at] = ghost_in[:modes]
    else:
        ghost[:, : 2 * ghosts] = ghost_in[:modes]
        ghost[:half, 2 * ghosts : tail_at] = ghost_in[rows - half :, :ghosts]
        ghost[half:, 2 * ghosts : tail_at] = ghost_in[rows - half : rows - 2 * half + modes, ghosts:]
    row = lax.broadcasted_iota(jnp.int32, (snaps, 128), 0)
    across = lax.broadcasted_iota(jnp.int32, (snaps, 128), 1)
    squares = jnp.zeros((snaps, count), F32)
    if pairs <= 4:
        for p in range(pairs):
            squares = whole_product(p, squares)
    else:
        squares = lax.fori_loop(0, pairs, whole_product, squares)

    norm = jnp.sum(jnp.sqrt(squares), axis=1, keepdims=True)
    norms[me] = jnp.sum(jnp.where(row == across, norm, 0.0), axis=0, keepdims=True)

    @pl.when(jnp.logical_not(climbing & top))
    def _():
        pl.semaphore_wait(known, 1)

    def norm_copy(j):
        return remote(norms.at[me], norms.at[me], send_c, recv_c, other(j))

    repeat(devices - 1, lambda j: norm_copy(j).start())

    def to_elem(j):
        to = me_e + (j + 1)
        to = jnp.where(to >= elems, to - elems, to)
        return remote(part_e.at[me_e], part_e.at[me_e], send_e, recv_e, dev(to, lead))

    def result(p):
        return remote(total_ref, total_ref, send_t.at[p], recv_t, dev(me_e, p))

    @pl.when(leading)
    def _():
        wait_bytes(part_p.at[pl.ds(0, params - 1)], recv_p)
        chip = part_p[0]
        for p in range(1, params):
            chip = chip + part_p[p]
        force = chip[:, wide:]
        force0 = force.astype(BF16)
        left = force - force0.astype(F32)
        force1 = left.astype(BF16)
        force2 = (left - force1.astype(F32)).astype(BF16)
        both = (((1,), (1,)), ((), ()))
        total = lax.dot_general(force2, ghost[...], both, preferred_element_type=F32)
        total = total + lax.dot_general(force1, ghost[...], both, preferred_element_type=F32)
        total = total + lax.dot_general(force0, ghost[...], both, preferred_element_type=F32)
        part_e[me_e] = chip[:, :wide]
        part_e[me_e, :, :modes] = chip[:, :modes] + total
        repeat(elems - 1, lambda j: to_elem(j).start())

    everyone = norms.at[pl.ds(0, devices - 1)]
    wait_bytes(everyone, recv_c)
    whole = norms[0]
    for d in range(1, devices):
        whole = whole + norms[d]
    diagonal = jnp.where(row == across, jnp.broadcast_to(whole, (snaps, 128)), 0.0)
    row_scale = jnp.sum(diagonal, axis=1, keepdims=True) / elem_total
    inverse = jnp.broadcast_to(1.0 / row_scale, (snaps, count))
    piece = cols_ref[...].reshape(modes, snaps, count) * inverse[None]
    training_ref[...] = piece.astype(BF16)

    every_elem = part_e.at[pl.ds(0, elems - 1)]

    @pl.when(leading)
    def _():
        wait_bytes(every_elem, recv_e)
        total = part_e[0]
        for e in range(1, elems):
            total = total + part_e[e]
        total_ref[...] = total
        for p in range(params - 1):
            result(p).start()

    @pl.when(jnp.logical_not(leading))
    def _():
        result(0).wait_recv()

    target_ref[...] = total_ref[:, :modes] / (row_scale * math.sqrt(elem_total))

    wait_bytes(others, send_n)
    wait_bytes(everyone, send_c)

    @pl.when(first)
    def _():
        to_relay().wait_send()

    @pl.when(jnp.logical_not(first))
    def _():
        wait_bytes(backs, send_d)

    @pl.when(relaying)
    def _():
        for q in range(params):
            wait_bytes(relay_disp, send_rd.at[q])
        ghost_from_relay().wait_send()

    @pl.when(leading)
    def _():
        ghost_copy().wait_send()
        for p in range(params - 1):
            hand_on(p).wait_send()
        wait_bytes(every_elem, send_e)
        for p in range(params - 1):
            result(p).wait_send()

    @pl.when(jnp.logical_not(leading))
    def _():
        to_lead().wait_send()


def finish_kernel(training_ref, target_ref, training_hbm, target_hbm, sem):
    copies = [
        pltpu.make_async_copy(target_ref, target_hbm, sem.at[0]),
        pltpu.make_async_copy(training_ref, training_hbm, sem.at[1]),
    ]
    for copy in copies:
        copy.start()
    for copy in copies:
        copy.wait()


def local(elems, params, coords, basis_rows, connectivity, modulus, stiffness):
    own_snaps, modes = coords.shape
    nodes = basis_rows.shape[2]
    count = connectivity.shape[0]
    snaps = own_snaps * params
    ghosts = nodes // 4
    if ghosts % 128 == 0:
        packed = (round_up(modes, 16), 3 * ghosts)
    else:
        packed = (round_up(modes, 16) + round_up(-(-modes // 2), 16), 2 * ghosts)
    edge = round_up(3 * ghosts + 32, 128)
    tiles = nodes // 128 + -(-ghosts // 128)
    wide = round_up(modes, 128)
    dofs = stiffness.shape[0]
    devices = elems * params
    inner = 4
    pairs = snaps // 2
    dma = pltpu.SemaphoreType.DMA
    vmem = pl.BlockSpec(memory_space=pltpu.VMEM)
    hbm = pl.BlockSpec(memory_space=pltpu.HBM)
    training, target = pl.pallas_call(
        functools.partial(kernel, elems, params, inner),
        out_shape=(
            jax.ShapeDtypeStruct((modes, snaps, count), BF16),
            jax.ShapeDtypeStruct((snaps, modes), F32),
        ),
        in_specs=[hbm] * 5,
        out_specs=(vmem, vmem),
        scratch_shapes=[
            pltpu.VMEM((own_snaps, modes), BF16),
            pltpu.VMEM((3, modes, nodes), BF16),
            pltpu.VMEM((8, count), jnp.int32),
            pltpu.VMEM((1, count), F32),
            pltpu.VMEM((dofs, dofs), F32),
            pltpu.VMEM(packed, BF16),
            pltpu.VMEM(packed, BF16),
            pltpu.VMEM((modes, edge), BF16),
            pltpu.VMEM((params, tiles, 3, own_snaps, 128), F32),
            pltpu.VMEM((pairs, dofs, 2 * count), F32),
            pltpu.VMEM((pairs if pairs <= 4 else 1, 3 * nodes, 2 * count), BF16),
            pltpu.VMEM((pairs, edge, 2 * count), BF16),
            pltpu.VMEM((pairs, modes, 2 * count), F32),
            pltpu.VMEM((modes * snaps, count), F32),
            pltpu.VMEM((wide, 128), F32),
            pltpu.VMEM((edge, 128), F32),
            pltpu.VMEM((devices, 1, 128), F32),
            pltpu.VMEM((params, snaps, wide + edge), F32),
            pltpu.VMEM((elems, snaps, wide), F32),
            pltpu.VMEM((snaps, wide), F32),
            pltpu.VMEM((params, tiles - nodes // 128, 3, own_snaps, 128), F32),
            pltpu.VMEM(packed, BF16),
            dma((4,)), dma, dma, dma, dma, dma, dma, dma, dma((params - 1,)), dma,
            dma, dma, dma, dma, dma, dma, dma((params - 1,)), dma,
            dma((params,)), dma, dma, dma,
            pltpu.SemaphoreType.REGULAR, pltpu.SemaphoreType.REGULAR,
        ],
        compiler_params=pltpu.CompilerParams(
            collective_id=0, has_side_effects=True, vmem_limit_bytes=40 * 1024 * 1024
        ),
    )(*(pltpu.with_memory_space_constraint(x, pltpu.HBM) for x in (
        coords, basis_rows, connectivity.T, modulus[None], stiffness
    )))
    training, target = pl.pallas_call(
        finish_kernel,
        out_shape=(
            jax.ShapeDtypeStruct((modes, snaps, count), BF16),
            jax.ShapeDtypeStruct((snaps, modes), F32),
        ),
        in_specs=[vmem, vmem],
        out_specs=(hbm, hbm),
        scratch_shapes=[dma((2,))],
        compiler_params=pltpu.CompilerParams(vmem_limit_bytes=20 * 1024 * 1024),
    )(training, target)
    return (jnp.transpose(training, (1, 0, 2)), target)


def solution(mesh):
    in_specs = (
        P("param", None),
        P(None, None, "elem"),
        P(("elem", "param"), None),
        P(("elem", "param")),
        P(),
    )
    out_specs = (P(None, None, ("elem", "param")), P())
    run = functools.partial(local, mesh.shape["elem"], mesh.shape["param"])
    return jax.shard_map(run, mesh=mesh, in_specs=in_specs, out_specs=out_specs, check_vma=False)
```

```python
import functools
import math

import jax
import jax.numpy as jnp
from jax import lax
from jax.experimental import pallas as pl
from jax.experimental.pallas import tpu as pltpu
from jax.sharding import PartitionSpec as P

LOGICAL = pl.DeviceIdType.LOGICAL
F32 = jnp.float32
BF16 = jnp.bfloat16
UNROLL = 64


def round_up(value, to):
    return -(-value // to) * to


def repeat(count, body):
    if count <= UNROLL:
        for j in range(count):
            body(j)
    else:
        lax.fori_loop(0, count, lambda j, c: (body(j), c)[1], 0)


def kernel(
    elems, params, inner,
    coords_hbm, basis_hbm, conn_hbm, modulus_hbm, stiff_hbm,
    cols_ref, inverse_ref, target_ref,
    coords_ref, basis_ref, conn_ref, modulus_ref, stiff_ref,
    packed, ghost_in, ghost, disp, corner_disp, weights, edge_weights, acc, part, nodal,
    norms, part_p, part_e, total_ref, relay_disp, relay_ghost,
    load, load_b, send_g, recv_g, send_d, recv_d, send_n, recv_n, send_f, recv_f,
    send_c, recv_c, send_p, recv_p, send_e, recv_e, send_t, recv_t,
    send_rd, recv_rd, send_rg, recv_rg, climb, known,
):
    own_snaps, modes = coords_hbm.shape
    dofs = stiff_hbm.shape[0]
    snaps = own_snaps * params
    pairs = snaps // 2
    nodes = basis_hbm.shape[2]
    ghosts = nodes // 4
    count = conn_hbm.shape[1]
    devices = elems * params
    outer = elems // inner
    elem_total = count * devices
    wide, edge = part_e.shape[2], ghost.shape[1]
    own_tiles = nodes // 128
    ghost_tiles = disp.shape[1] - own_tiles
    me_e, me_p = lax.axis_index("elem"), lax.axis_index("param")
    me = me_e * params + me_p
    lead = params - 1
    leading = me_p == lead
    first, last = me_e == 0, me_e == elems - 1
    before = jnp.where(first, elems - 1, me_e - 1)
    relay = (elems // 4 + 1) * params + lead
    relaying = me == relay
    me_o, me_i = lax.div(me_e, inner), lax.rem(me_e, inner)
    bottom, top = me_o == 0, me_o == outer - 1
    climbing = me_p == 0

    def dev(e, p):
        return e * params + p

    def other(j):
        to = me + (j + 1)
        return jnp.where(to >= devices, to - devices, to)

    def signal(semaphore, device):
        pl.semaphore_signal(semaphore, inc=1, device_id=device, device_id_type=LOGICAL)

    def remote(src, dst, send, recv, device):
        return pltpu.make_async_remote_copy(
            src_ref=src, dst_ref=dst, send_sem=send, recv_sem=recv,
            device_id=device, device_id_type=LOGICAL,
        )

    def wait_bytes(ref, semaphore):
        pltpu.make_async_copy(ref, ref, semaphore).wait()

    load_basis = pltpu.make_async_copy(basis_hbm, basis_ref, load_b)
    smalls = [
        pltpu.make_async_copy(src, dst, load.at[i])
        for i, (src, dst) in enumerate([
            (coords_hbm, coords_ref), (conn_hbm, conn_ref),
            (modulus_hbm, modulus_ref), (stiff_hbm, stiff_ref),
        ])
    ]
    for copy in [load_basis] + smalls:
        copy.start()

    barrier = pltpu.get_barrier_semaphore()
    @pl.when(first | last)
    def _():
        signal(barrier, relay)

    @pl.when(relaying)
    def _():
        for p in range(params):
            signal(barrier, dev(elems - 1, p))
            signal(barrier, dev(0, p))

    @pl.when(jnp.logical_not(first))
    def _():
        for p in range(params):
            signal(barrier, dev(me_e - 1, p))

    @pl.when(jnp.logical_not(last))
    def _():
        for p in range(params):
            signal(barrier, dev(me_e + 1, p))

    @pl.when(climbing & jnp.logical_not(bottom))
    def _():
        signal(barrier, dev(me_e - inner, 0))

    @pl.when(climbing & jnp.logical_not(top))
    def _():
        signal(barrier, dev(me_e + inner, 0))

    for j in range(1, params):
        to = me_p + j
        signal(barrier, dev(me_e, jnp.where(to >= params, to - params, to)))
    for j in range(1, inner):
        to = me_i + j
        signal(barrier, dev(me_o * inner + jnp.where(to >= inner, to - inner, to), 0))
    greeted = params - 1 + jnp.where(first | last, 1, params) + params
    greeted += jnp.where(relaying, 2 * params, 0)
    climbs = (inner - 1) * params + 2 - jnp.where(bottom | top, 1, 0)
    greeted += jnp.where(climbing, climbs, 0)

    part[...] = jnp.zeros_like(part)
    nodal[...] = jnp.zeros_like(nodal)
    tail_at = 3 * ghosts
    for p in range(pairs):
        edge_weights[p, tail_at:] = jnp.zeros((edge - tail_at, 2 * count), BF16)
    for copy in smalls:
        copy.wait()
    coords = coords_ref[...]
    load_basis.wait()
    for k in range(3):
        moved = jnp.dot(coords, basis_ref[k], preferred_element_type=F32)
        moved = moved.astype(BF16).astype(F32)
        for t in range(own_tiles):
            disp[me_p, t, k] = moved[:, t * 128 : (t + 1) * 128]
    rows = packed.shape[0]
    if ghosts % 128 == 0:
        for k in range(3):
            packed[:modes, k * ghosts : (k + 1) * ghosts] = basis_ref[k, :, :ghosts]
    else:
        half = rows - round_up(modes, 16)
        packed[:modes, :ghosts] = basis_ref[0, :, :ghosts]
        packed[:modes, ghosts:] = basis_ref[1, :, :ghosts]
        packed[rows - half :, :ghosts] = basis_ref[2, :half, :ghosts]
        packed[rows - half : rows - 2 * half + modes, ghosts:] = basis_ref[2, half:, :ghosts]

    pl.semaphore_wait(barrier, greeted)
    own_part, ghost_part = pl.ds(0, own_tiles), pl.ds(own_tiles, ghost_tiles)
    front = disp.at[me_p, pl.ds(0, ghost_tiles)]
    backs = disp.at[:, ghost_part]

    def ghost_disp(p):
        turn = lax.rem(me_p + p, params)
        return remote(front, disp.at[me_p, ghost_part], send_d, recv_d, dev(before, turn))

    def own_disp(p):
        turn = lax.rem(me_p + p, params)
        mine = disp.at[me_p, own_part]
        return remote(mine, mine, send_n, recv_n, dev(me_e, turn))

    def to_relay():
        return remote(front, relay_disp.at[me_p], send_d, recv_rd, relay)

    def from_relay(q, p):
        return remote(
            relay_disp.at[q], disp.at[q, ghost_part], send_rd.at[q], recv_d, dev(elems - 1, p)
        )

    def ghost_copy():
        return remote(packed, ghost_in, send_g, recv_g, dev(before, lead))

    def ghost_to_relay():
        return remote(packed, relay_ghost, send_g, recv_rg, relay)

    def ghost_from_relay():
        return remote(relay_ghost, ghost_in, send_rg, recv_g, dev(elems - 1, lead))

    def hand_on(p):
        return remote(ghost_in, ghost_in, send_f.at[p], recv_f, dev(me_e, p))

    @pl.when(first)
    def _():
        to_relay().start()

    @pl.when(jnp.logical_not(first))
    def _():
        for p in range(params):
            ghost_disp(p).start()

    @pl.when(first & leading)
    def _():
        ghost_to_relay().start()

    @pl.when(jnp.logical_not(first) & leading)
    def _():
        ghost_copy().start()

    for p in range(1, params):
        own_disp(p).start()

    @pl.when(relaying)
    def _():
        wait_bytes(relay_disp, recv_rd)
        for q in range(params):
            for p in range(params):
                from_relay(q, params - 1 - p).start()
        ghost_to_relay().wait_recv()
        ghost_from_relay().start()

    @pl.when(climbing & jnp.logical_not(bottom))
    def _():
        pl.semaphore_wait(climb, 1)

    @pl.when(climbing & jnp.logical_not(top))
    def _():
        signal(climb, dev(me_e + inner, 0))

    @pl.when(climbing & top)
    def _():
        for p in range(1, params):
            signal(known, dev(me_e, p))
        for o in range(outer - 1):
            for p in range(params):
                signal(known, dev(o * inner + me_i, p))

    corners = conn_ref[...]
    base = jnp.min(corners, axis=0, keepdims=True)
    residue = corners % 8
    lane_at = corners % 128
    tile_at = corners // 128
    row8 = lax.broadcasted_iota(jnp.int32, (8, count), 0)
    lane = lax.broadcasted_iota(jnp.int32, (1, 128), 1)
    hits = [residue[a : a + 1] == row8 for a in range(8)]

    def inside(start, height):
        node = start + lax.broadcasted_iota(jnp.int32, (height, count), 0)
        return (node >= base) & (node < base + 8)

    own_rows = lax.broadcasted_iota(jnp.int32, (nodes, count), 0) < nodes - 8
    own_mask = jnp.where(inside(0, nodes) & own_rows, 1.0, 0.0).astype(BF16)
    ghost_mask = jnp.where(inside(nodes, ghosts), 1.0, 0.0)
    tail_mask = jnp.where(inside(nodes - 8, 8), 1.0, 0.0)
    stiff = stiff_ref[...]
    high = stiff.astype(BF16)
    rest = stiff - high.astype(F32)
    mid = rest.astype(BF16)
    low = (rest - mid.astype(F32)).astype(BF16)
    modulus = modulus_ref[...]
    modulus2 = jnp.concatenate([modulus, modulus], axis=1)
    tails = [basis_ref[k, :, nodes - 8 :] for k in range(3)]
    start = tail_at // 128 * 128
    blank = [jnp.zeros((modes, tail_at - start), BF16)] if tail_at > start else []
    after = [jnp.zeros((modes, edge - tail_at - 24), BF16)]
    ghost[:, start:] = jnp.concatenate(blank + tails + after, axis=1)

    def gathered(p, found, tiles):
        pieces = []
        for at in range(2):
            s = 2 * p + at
            parts = []
            for k in range(3):
                piece = found[k * 8 : (k + 1) * 8, at * count : (at + 1) * count]
                for t in tiles:
                    line = disp[s // own_snaps, t, k, pl.ds(s % own_snaps, 1), :]
                    got = jnp.take_along_axis(jnp.broadcast_to(line, (8, 128)), lane_at, axis=1)
                    piece = jnp.where(tile_at == t, got, piece)
                parts.append(piece)
            pieces.append(jnp.concatenate(parts, axis=0))
        return jnp.concatenate(pieces, axis=1)

    def forces_of(moved):
        moved16 = moved.astype(BF16)
        linear = jnp.dot(low, moved16, preferred_element_type=F32)
        linear = linear + jnp.dot(mid, moved16, preferred_element_type=F32)
        linear = linear + jnp.dot(high, moved16, preferred_element_type=F32)
        return (modulus2 * (linear + 0.25 * moved * moved * moved)).astype(BF16).astype(F32)

    def spread_of(forces, at, k):
        spread = jnp.zeros((8, count), F32)
        for a in range(8):
            force = forces[k * 8 + a : k * 8 + a + 1, at * count : (at + 1) * count]
            spread = spread + jnp.where(hits[a], force, 0.0)
        return spread.astype(BF16).astype(F32)

    def own_product(p):
        slot = p if weights.shape[0] > 1 else 0
        moved = gathered(p, jnp.zeros((dofs, 2 * count), F32), range(own_tiles))
        corner_disp[p] = moved
        forces = forces_of(moved)
        for at in range(2):
            columns = slice(at * count, (at + 1) * count)
            for k in range(3):
                spread = spread_of(forces, at, k)
                twice = jnp.concatenate([spread, spread], axis=0).astype(BF16)
                tall = jnp.concatenate([twice] * (nodes // 16), axis=0) * own_mask
                weights[slot, k * nodes : (k + 1) * nodes, columns] = tall
        total = jnp.dot(basis_ref[0], weights[slot, :nodes], preferred_element_type=F32)
        for k in range(1, 3):
            total = total + jnp.dot(
                basis_ref[k], weights[slot, k * nodes : (k + 1) * nodes], preferred_element_type=F32
            )
        acc[p] = total

    def own_sums(p):
        for at in range(2):
            mine = acc[p, :, at * count : (at + 1) * count]
            total = jnp.sum(mine, axis=1, keepdims=True)
            part[:modes] = jnp.where(lane == 2 * p + at, total, part[:modes])

    def edge_forces(p):
        moved = gathered(p, corner_disp[p], range(own_tiles, own_tiles + ghost_tiles))
        forces = forces_of(moved)
        for at in range(2):
            columns = slice(at * count, (at + 1) * count)
            ends = []
            for k in range(3):
                spread = spread_of(forces, at, k)
                tall = jnp.concatenate([spread] * (ghosts // 8), axis=0) * ghost_mask
                edge_weights[p, k * ghosts : (k + 1) * ghosts, columns] = tall.astype(BF16)
                ends.append(spread * tail_mask)
                total = jnp.sum(tall, axis=1, keepdims=True)
                at_rows = slice(k * ghosts, (k + 1) * ghosts)
                nodal[at_rows] = jnp.where(lane == 2 * p + at, total, nodal[at_rows])
            end = jnp.concatenate(ends + [jnp.zeros((8, count), F32)], axis=0)
            edge_weights[p, tail_at : tail_at + 32, columns] = end.astype(BF16)
            total = jnp.sum(end, axis=1, keepdims=True)
            at_rows = slice(tail_at, tail_at + 32)
            nodal[at_rows] = jnp.where(lane == 2 * p + at, total, nodal[at_rows])

    def whole_product(p, squares):
        result = acc[p] + jnp.dot(ghost[...], edge_weights[p], preferred_element_type=F32)
        for at in range(2):
            s = 2 * p + at
            mine = result[:, at * count : (at + 1) * count]
            cols_ref[pl.ds(s, modes, stride=snaps), :] = mine
            norm = jnp.sum(mine * mine, axis=0, keepdims=True)
            squares = jnp.where(row == s, norm, squares)
        return squares

    def each_pair(body):
        if pairs <= 4:
            for p in range(pairs):
                body(p)
        else:
            lax.fori_loop(0, pairs, lambda p, c: (body(p), c)[1], 0)

    others = disp.at[pl.ds(0, params - 1), own_part]
    wait_bytes(others, recv_n)
    each_pair(own_product)
    each_pair(own_sums)

    def flipped(ref):
        return jnp.concatenate(
            [jnp.transpose(ref[t * 128 : (t + 1) * 128])[:snaps] for t in range(ref.shape[0] // 128)],
            axis=1,
        )

    part_p[me_p, :, :wide] = flipped(part)
    wait_bytes(backs, recv_d)
    each_pair(edge_forces)
    part_p[me_p, :, wide:] = flipped(nodal)

    def to_lead():
        return remote(part_p.at[me_p], part_p.at[me_p], send_p, recv_p, dev(me_e, lead))

    @pl.when(jnp.logical_not(leading))
    def _():
        to_lead().start()

    @pl.when(leading)
    def _():
        ghost_copy().wait_recv()
        for p in range(params - 1):
            hand_on(p).start()

    @pl.when(jnp.logical_not(leading))
    def _():
        hand_on(0).wait_recv()

    if ghosts % 128 == 0:
        ghost[:, :tail_at] = ghost_in[:modes]
    else:
        ghost[:, : 2 * ghosts] = ghost_in[:modes]
        ghost[:half, 2 * ghosts : tail_at] = ghost_in[rows - half :, :ghosts]
        ghost[half:, 2 * ghosts : tail_at] = ghost_in[rows - half : rows - 2 * half + modes, ghosts:]
    row = lax.broadcasted_iota(jnp.int32, (snaps, 128), 0)
    across = lax.broadcasted_iota(jnp.int32, (snaps, 128), 1)
    squares = jnp.zeros((snaps, count), F32)
    if pairs <= 4:
        for p in range(pairs):
            squares = whole_product(p, squares)
    else:
        squares = lax.fori_loop(0, pairs, whole_product, squares)

    norm = jnp.sum(jnp.sqrt(squares), axis=1, keepdims=True)
    norms[me] = jnp.sum(jnp.where(row == across, norm, 0.0), axis=0, keepdims=True)

    @pl.when(jnp.logical_not(climbing & top))
    def _():
        pl.semaphore_wait(known, 1)

    def norm_copy(j):
        return remote(norms.at[me], norms.at[me], send_c, recv_c, other(j))

    repeat(devices - 1, lambda j: norm_copy(j).start())

    def to_elem(j):
        to = me_e + (j + 1)
        to = jnp.where(to >= elems, to - elems, to)
        return remote(part_e.at[me_e], part_e.at[me_e], send_e, recv_e, dev(to, lead))

    every_elem = part_e.at[pl.ds(0, elems - 1)]

    def result(p):
        return remote(total_ref, total_ref, send_t.at[p], recv_t, dev(me_e, p))

    @pl.when(leading)
    def _():
        wait_bytes(part_p.at[pl.ds(0, params - 1)], recv_p)
        chip = part_p[0]
        for p in range(1, params):
            chip = chip + part_p[p]
        force = chip[:, wide:]
        force0 = force.astype(BF16)
        left = force - force0.astype(F32)
        force1 = left.astype(BF16)
        force2 = (left - force1.astype(F32)).astype(BF16)
        both = (((1,), (1,)), ((), ()))
        total = lax.dot_general(force2, ghost[...], both, preferred_element_type=F32)
        total = total + lax.dot_general(force1, ghost[...], both, preferred_element_type=F32)
        total = total + lax.dot_general(force0, ghost[...], both, preferred_element_type=F32)
        part_e[me_e] = chip[:, :wide]
        part_e[me_e, :, :modes] = chip[:, :modes] + total
        repeat(elems - 1, lambda j: to_elem(j).start())
        wait_bytes(every_elem, recv_e)
        total = part_e[0]
        for e in range(1, elems):
            total = total + part_e[e]
        total_ref[...] = total
        for p in range(params - 1):
            result(p).start()

    everyone = norms.at[pl.ds(0, devices - 1)]
    wait_bytes(everyone, recv_c)
    whole = norms[0]
    for d in range(1, devices):
        whole = whole + norms[d]
    diagonal = jnp.where(row == across, jnp.broadcast_to(whole, (snaps, 128)), 0.0)
    row_scale = jnp.sum(diagonal, axis=1, keepdims=True) / elem_total
    inverse_ref[...] = jnp.broadcast_to(1.0 / row_scale, (snaps, count))

    @pl.when(jnp.logical_not(leading))
    def _():
        result(0).wait_recv()

    target_ref[...] = total_ref[:, :modes] / (row_scale * math.sqrt(elem_total))

    wait_bytes(others, send_n)
    wait_bytes(everyone, send_c)

    @pl.when(first)
    def _():
        to_relay().wait_send()

    @pl.when(jnp.logical_not(first))
    def _():
        wait_bytes(backs, send_d)

    @pl.when(relaying)
    def _():
        for q in range(params):
            wait_bytes(relay_disp, send_rd.at[q])
        ghost_from_relay().wait_send()

    @pl.when(leading)
    def _():
        ghost_copy().wait_send()
        for p in range(params - 1):
            hand_on(p).wait_send()
        wait_bytes(every_elem, send_e)
        for p in range(params - 1):
            result(p).wait_send()

    @pl.when(jnp.logical_not(leading))
    def _():
        to_lead().wait_send()


def finish_kernel(cols_ref, inverse_ref, target_ref, training_hbm, target_hbm, training, sem):
    modes, snaps, count = training.shape
    copies = [pltpu.make_async_copy(target_ref, target_hbm, sem.at[0])]
    copies[0].start()
    inverse = inverse_ref[...][None]
    chunks = sem.shape[0] - 1
    size = modes // chunks
    for c in range(chunks):
        rows = pl.ds(c * size, size)
        piece = cols_ref[c * size * snaps : (c + 1) * size * snaps]
        training[rows] = (piece.reshape(size, snaps, count) * inverse).astype(BF16)
        copies.append(pltpu.make_async_copy(training.at[rows], training_hbm.at[rows], sem.at[c + 1]))
        copies[-1].start()
    for copy in copies:
        copy.wait()


def local(elems, params, coords, basis_rows, connectivity, modulus, stiffness):
    own_snaps, modes = coords.shape
    nodes = basis_rows.shape[2]
    count = connectivity.shape[0]
    snaps = own_snaps * params
    ghosts = nodes // 4
    if ghosts % 128 == 0:
        packed = (round_up(modes, 16), 3 * ghosts)
    else:
        packed = (round_up(modes, 16) + round_up(-(-modes // 2), 16), 2 * ghosts)
    edge = round_up(3 * ghosts + 32, 128)
    tiles = nodes // 128 + -(-ghosts // 128)
    wide = round_up(modes, 128)
    dofs = stiffness.shape[0]
    devices = elems * params
    inner = 4
    pairs = snaps // 2
    dma = pltpu.SemaphoreType.DMA
    vmem = pl.BlockSpec(memory_space=pltpu.VMEM)
    hbm = pl.BlockSpec(memory_space=pltpu.HBM)
    cols, inverse, target = pl.pallas_call(
        functools.partial(kernel, elems, params, inner),
        out_shape=(
            jax.ShapeDtypeStruct((modes * snaps, count), F32),
            jax.ShapeDtypeStruct((snaps, count), F32),
            jax.ShapeDtypeStruct((snaps, modes), F32),
        ),
        in_specs=[hbm] * 5,
        out_specs=(vmem, vmem, vmem),
        scratch_shapes=[
            pltpu.VMEM((own_snaps, modes), BF16),
            pltpu.VMEM((3, modes, nodes), BF16),
            pltpu.VMEM((8, count), jnp.int32),
            pltpu.VMEM((1, count), F32),
            pltpu.VMEM((dofs, dofs), F32),
            pltpu.VMEM(packed, BF16),
            pltpu.VMEM(packed, BF16),
            pltpu.VMEM((modes, edge), BF16),
            pltpu.VMEM((params, tiles, 3, own_snaps, 128), F32),
            pltpu.VMEM((pairs, dofs, 2 * count), F32),
            pltpu.VMEM((pairs if pairs <= 4 else 1, 3 * nodes, 2 * count), BF16),
            pltpu.VMEM((pairs, edge, 2 * count), BF16),
            pltpu.VMEM((pairs, modes, 2 * count), F32),
            pltpu.VMEM((wide, 128), F32),
            pltpu.VMEM((edge, 128), F32),
            pltpu.VMEM((devices, 1, 128), F32),
            pltpu.VMEM((params, snaps, wide + edge), F32),
            pltpu.VMEM((elems, snaps, wide), F32),
            pltpu.VMEM((snaps, wide), F32),
            pltpu.VMEM((params, tiles - nodes // 128, 3, own_snaps, 128), F32),
            pltpu.VMEM(packed, BF16),
            dma((4,)), dma, dma, dma, dma, dma, dma, dma, dma((params - 1,)), dma,
            dma, dma, dma, dma, dma, dma, dma((params - 1,)), dma,
            dma((params,)), dma, dma, dma,
            pltpu.SemaphoreType.REGULAR, pltpu.SemaphoreType.REGULAR,
        ],
        compiler_params=pltpu.CompilerParams(
            collective_id=0, has_side_effects=True, vmem_limit_bytes=40 * 1024 * 1024
        ),
    )(*(pltpu.with_memory_space_constraint(x, pltpu.HBM) for x in (
        coords, basis_rows, connectivity.T, modulus[None], stiffness
    )))
    chunks = next(c for c in (4, 3, 2, 1) if modes % c == 0)
    training, target = pl.pallas_call(
        finish_kernel,
        out_shape=(
            jax.ShapeDtypeStruct((modes, snaps, count), BF16),
            jax.ShapeDtypeStruct((snaps, modes), F32),
        ),
        in_specs=[vmem, vmem, vmem],
        out_specs=(hbm, hbm),
        scratch_shapes=[pltpu.VMEM((modes, snaps, count), BF16), dma((chunks + 1,))],
        compiler_params=pltpu.CompilerParams(vmem_limit_bytes=20 * 1024 * 1024),
    )(cols, inverse, target)
    return (jnp.transpose(training, (1, 0, 2)), target)


def solution(mesh):
    in_specs = (
        P("param", None),
        P(None, None, "elem"),
        P(("elem", "param"), None),
        P(("elem", "param")),
        P(),
    )
    out_specs = (P(None, None, ("elem", "param")), P())
    run = functools.partial(local, mesh.shape["elem"], mesh.shape["param"])
    return jax.shard_map(run, mesh=mesh, in_specs=in_specs, out_specs=out_specs, check_vma=False)
```

```python
import functools
import math

import jax
import jax.numpy as jnp
from jax import lax
from jax.experimental import pallas as pl
from jax.experimental.pallas import tpu as pltpu
from jax.sharding import PartitionSpec as P

LOGICAL = pl.DeviceIdType.LOGICAL
F32 = jnp.float32
BF16 = jnp.bfloat16
UNROLL = 64
CHUNKS = 4


def round_up(value, to):
    return -(-value // to) * to


def repeat(count, body):
    if count <= UNROLL:
        for j in range(count):
            body(j)
    else:
        lax.fori_loop(0, count, lambda j, c: (body(j), c)[1], 0)


def kernel(
    elems, params, inner,
    coords_hbm, basis_hbm, conn_hbm, modulus_hbm, stiff_hbm,
    cols_ref, inverse_ref, target_ref,
    coords_ref, basis_ref, conn_ref, modulus_ref, stiff_ref,
    packed, ghost_in, ghost, disp, corner_disp, weights, edge_weights, acc, part, nodal,
    norms, part_p, part_e, total_ref, relay_disp, relay_ghost,
    load, load_b, send_g, recv_g, recv_d, recv_n, send_f, recv_f,
    recv_c, recv_p, recv_e, send_t, recv_t,
    send_rd, recv_rd, send_rg, recv_rg, climb, known,
):
    send_d, send_n, send_p, send_e = [load.at[i] for i in range(4)]
    send_c = load_b
    own_snaps, modes = coords_hbm.shape
    dofs = stiff_hbm.shape[0]
    snaps = own_snaps * params
    pairs = snaps // 2
    nodes = basis_hbm.shape[2]
    ghosts = nodes // 4
    count = conn_hbm.shape[1]
    devices = elems * params
    outer = elems // inner
    elem_total = count * devices
    wide, edge = part_e.shape[2], ghost.shape[1]
    own_tiles = nodes // 128
    ghost_tiles = disp.shape[1] - own_tiles
    me_e, me_p = lax.axis_index("elem"), lax.axis_index("param")
    me = me_e * params + me_p
    lead = params - 1
    leading = me_p == lead
    first, last = me_e == 0, me_e == elems - 1
    before = jnp.where(first, elems - 1, me_e - 1)
    relay = (elems // 4 + 1) * params + lead
    relaying = me == relay
    me_o, me_i = lax.div(me_e, inner), lax.rem(me_e, inner)
    bottom, top = me_o == 0, me_o == outer - 1
    guide = inner // 2
    climbing = (me_p == 0) & (me_i == guide)

    def dev(e, p):
        return e * params + p

    def other(j):
        to = me + (j + 1)
        return jnp.where(to >= devices, to - devices, to)

    def signal(semaphore, device):
        pl.semaphore_signal(semaphore, inc=1, device_id=device, device_id_type=LOGICAL)

    def remote(src, dst, send, recv, device):
        return pltpu.make_async_remote_copy(
            src_ref=src, dst_ref=dst, send_sem=send, recv_sem=recv,
            device_id=device, device_id_type=LOGICAL,
        )

    def wait_bytes(ref, semaphore):
        pltpu.make_async_copy(ref, ref, semaphore).wait()

    load_basis = pltpu.make_async_copy(basis_hbm, basis_ref, load_b)
    smalls = [
        pltpu.make_async_copy(src, dst, load.at[i])
        for i, (src, dst) in enumerate([
            (coords_hbm, coords_ref), (conn_hbm, conn_ref),
            (modulus_hbm, modulus_ref), (stiff_hbm, stiff_ref),
        ])
    ]
    for copy in [load_basis] + smalls:
        copy.start()

    barrier = pltpu.get_barrier_semaphore()
    @pl.when(first | last)
    def _():
        signal(barrier, relay)

    @pl.when(relaying)
    def _():
        for p in range(params):
            signal(barrier, dev(elems - 1, p))
            signal(barrier, dev(0, p))

    @pl.when(jnp.logical_not(first))
    def _():
        for p in range(params):
            signal(barrier, dev(me_e - 1, p))

    @pl.when(jnp.logical_not(last))
    def _():
        for p in range(params):
            signal(barrier, dev(me_e + 1, p))

    @pl.when(climbing & jnp.logical_not(bottom))
    def _():
        signal(barrier, dev(me_e - inner, 0))

    @pl.when(climbing & jnp.logical_not(top))
    def _():
        signal(barrier, dev(me_e + inner, 0))

    for j in range(1, params):
        to = me_p + j
        signal(barrier, dev(me_e, jnp.where(to >= params, to - params, to)))

    @pl.when(me_i != guide)
    def _():
        signal(barrier, dev(me_o * inner + guide, 0))

    greeted = params - 1 + jnp.where(first | last, 1, params) + params
    greeted += jnp.where(relaying, 2 * params, 0)
    climbs = (inner - 1) * params + 2 - jnp.where(bottom | top, 1, 0)
    greeted += jnp.where(climbing, climbs, 0)

    part[...] = jnp.zeros_like(part)
    nodal[...] = jnp.zeros_like(nodal)
    tail_at = 3 * ghosts
    for p in range(pairs):
        edge_weights[p, tail_at:] = jnp.zeros((edge - tail_at, 2 * count), BF16)
    for copy in smalls:
        copy.wait()
    coords = coords_ref[...]
    load_basis.wait()
    for k in range(3):
        moved = jnp.dot(coords, basis_ref[k], preferred_element_type=F32)
        moved = moved.astype(BF16).astype(F32)
        for t in range(own_tiles):
            disp[me_p, t, k] = moved[:, t * 128 : (t + 1) * 128]
    rows = packed.shape[0]
    if ghosts % 128 == 0:
        for k in range(3):
            packed[:modes, k * ghosts : (k + 1) * ghosts] = basis_ref[k, :, :ghosts]
    else:
        half = rows - round_up(modes, 16)
        packed[:modes, :ghosts] = basis_ref[0, :, :ghosts]
        packed[:modes, ghosts:] = basis_ref[1, :, :ghosts]
        packed[rows - half :, :ghosts] = basis_ref[2, :half, :ghosts]
        packed[rows - half : rows - 2 * half + modes, ghosts:] = basis_ref[2, half:, :ghosts]

    pl.semaphore_wait(barrier, greeted)
    own_part, ghost_part = pl.ds(0, own_tiles), pl.ds(own_tiles, ghost_tiles)
    front = disp.at[me_p, pl.ds(0, ghost_tiles)]
    backs = disp.at[:, ghost_part]

    def ghost_disp(p):
        turn = lax.rem(me_p + p, params)
        return remote(front, disp.at[me_p, ghost_part], send_d, recv_d, dev(before, turn))

    def own_disp(p):
        turn = lax.rem(me_p + p, params)
        mine = disp.at[me_p, own_part]
        return remote(mine, mine, send_n, recv_n, dev(me_e, turn))

    def to_relay():
        return remote(front, relay_disp.at[me_p], send_d, recv_rd, relay)

    def from_relay(q, p):
        return remote(
            relay_disp.at[q], disp.at[q, ghost_part], send_rd.at[q], recv_d, dev(elems - 1, p)
        )

    cuts = [rows // 16 * c // CHUNKS * 16 for c in range(CHUNKS + 1)]

    def cut(ref, c):
        return ref.at[pl.ds(cuts[c], cuts[c + 1] - cuts[c])]

    def ghost_copy(c):
        return remote(cut(packed, c), cut(ghost_in, c), send_g, recv_g.at[c], dev(before, lead))

    def ghost_to_relay(c):
        return remote(cut(packed, c), cut(relay_ghost, c), send_g, recv_rg.at[c], relay)

    def ghost_from_relay(c):
        return remote(
            cut(relay_ghost, c), cut(ghost_in, c), send_rg, recv_g.at[c], dev(elems - 1, lead)
        )

    def hand_on(p, c):
        return remote(cut(ghost_in, c), cut(ghost_in, c), send_f.at[p], recv_f, dev(me_e, p))

    @pl.when(first)
    def _():
        to_relay().start()

    @pl.when(jnp.logical_not(first))
    def _():
        for p in range(params):
            ghost_disp(p).start()

    @pl.when(first & leading)
    def _():
        for c in range(CHUNKS):
            ghost_to_relay(c).start()

    @pl.when(jnp.logical_not(first) & leading)
    def _():
        for c in range(CHUNKS):
            ghost_copy(c).start()

    for p in range(1, params):
        own_disp(p).start()

    @pl.when(relaying)
    def _():
        wait_bytes(relay_disp, recv_rd)
        for q in range(params):
            for p in range(params):
                from_relay(q, p).start()
        for c in range(CHUNKS):
            ghost_to_relay(c).wait_recv()
            ghost_from_relay(c).start()

    @pl.when(climbing & jnp.logical_not(bottom))
    def _():
        pl.semaphore_wait(climb, 1)

    @pl.when(climbing & jnp.logical_not(top))
    def _():
        signal(climb, dev(me_e + inner, 0))

    @pl.when(climbing & top)
    def _():
        repeat(devices - 1, lambda j: signal(known, other(j)))

    corners = conn_ref[...]
    base = jnp.min(corners, axis=0, keepdims=True)
    residue = corners % 8
    lane_at = corners % 128
    tile_at = corners // 128
    row8 = lax.broadcasted_iota(jnp.int32, (8, count), 0)
    lane = lax.broadcasted_iota(jnp.int32, (1, 128), 1)
    hits = [residue[a : a + 1] == row8 for a in range(8)]

    def inside(start, height):
        node = start + lax.broadcasted_iota(jnp.int32, (height, count), 0)
        return (node >= base) & (node < base + 8)

    own_rows = lax.broadcasted_iota(jnp.int32, (nodes, count), 0) < nodes - 8
    own_mask = jnp.where(inside(0, nodes) & own_rows, 1.0, 0.0).astype(BF16)
    ghost_mask = jnp.where(inside(nodes, ghosts), 1.0, 0.0)
    tail_mask = jnp.where(inside(nodes - 8, 8), 1.0, 0.0)
    stiff = stiff_ref[...]
    high = stiff.astype(BF16)
    rest = stiff - high.astype(F32)
    mid = rest.astype(BF16)
    low = (rest - mid.astype(F32)).astype(BF16)
    modulus = modulus_ref[...]
    modulus2 = jnp.concatenate([modulus, modulus], axis=1)
    tails = [basis_ref[k, :, nodes - 8 :] for k in range(3)]
    start = tail_at // 128 * 128
    blank = [jnp.zeros((modes, tail_at - start), BF16)] if tail_at > start else []
    after = [jnp.zeros((modes, edge - tail_at - 24), BF16)]
    ghost[:, start:] = jnp.concatenate(blank + tails + after, axis=1)

    def gathered(p, found, tiles):
        pieces = []
        for at in range(2):
            s = 2 * p + at
            parts = []
            for k in range(3):
                piece = found[k * 8 : (k + 1) * 8, at * count : (at + 1) * count]
                for t in tiles:
                    line = disp[s // own_snaps, t, k, pl.ds(s % own_snaps, 1), :]
                    got = jnp.take_along_axis(jnp.broadcast_to(line, (8, 128)), lane_at, axis=1)
                    piece = jnp.where(tile_at == t, got, piece)
                parts.append(piece)
            pieces.append(jnp.concatenate(parts, axis=0))
        return jnp.concatenate(pieces, axis=1)

    def forces_of(moved):
        moved16 = moved.astype(BF16)
        linear = jnp.dot(low, moved16, preferred_element_type=F32)
        linear = linear + jnp.dot(mid, moved16, preferred_element_type=F32)
        linear = linear + jnp.dot(high, moved16, preferred_element_type=F32)
        return (modulus2 * (linear + 0.25 * moved * moved * moved)).astype(BF16).astype(F32)

    def spread_of(forces, at, k):
        spread = jnp.zeros((8, count), F32)
        for a in range(8):
            force = forces[k * 8 + a : k * 8 + a + 1, at * count : (at + 1) * count]
            spread = spread + jnp.where(hits[a], force, 0.0)
        return spread.astype(BF16).astype(F32)

    def own_product(p):
        slot = p if weights.shape[0] > 1 else 0
        moved = gathered(p, jnp.zeros((dofs, 2 * count), F32), range(own_tiles))
        corner_disp[p] = moved
        forces = forces_of(moved)
        for at in range(2):
            columns = slice(at * count, (at + 1) * count)
            for k in range(3):
                spread = spread_of(forces, at, k)
                twice = jnp.concatenate([spread, spread], axis=0).astype(BF16)
                tall = jnp.concatenate([twice] * (nodes // 16), axis=0) * own_mask
                weights[slot, k * nodes : (k + 1) * nodes, columns] = tall
        total = jnp.dot(basis_ref[0], weights[slot, :nodes], preferred_element_type=F32)
        for k in range(1, 3):
            total = total + jnp.dot(
                basis_ref[k], weights[slot, k * nodes : (k + 1) * nodes], preferred_element_type=F32
            )
        acc[p] = total

    def own_sums(p):
        for at in range(2):
            mine = acc[p, :, at * count : (at + 1) * count]
            total = jnp.sum(mine, axis=1, keepdims=True)
            part[:modes] = jnp.where(lane == 2 * p + at, total, part[:modes])

    def edge_forces(p):
        moved = gathered(p, corner_disp[p], range(own_tiles, own_tiles + ghost_tiles))
        forces = forces_of(moved)
        for at in range(2):
            columns = slice(at * count, (at + 1) * count)
            ends = []
            for k in range(3):
                spread = spread_of(forces, at, k)
                tall = jnp.concatenate([spread] * (ghosts // 8), axis=0) * ghost_mask
                edge_weights[p, k * ghosts : (k + 1) * ghosts, columns] = tall.astype(BF16)
                ends.append(spread * tail_mask)
                total = jnp.sum(tall, axis=1, keepdims=True)
                at_rows = slice(k * ghosts, (k + 1) * ghosts)
                nodal[at_rows] = jnp.where(lane == 2 * p + at, total, nodal[at_rows])
            end = jnp.concatenate(ends + [jnp.zeros((8, count), F32)], axis=0)
            edge_weights[p, tail_at : tail_at + 32, columns] = end.astype(BF16)
            total = jnp.sum(end, axis=1, keepdims=True)
            at_rows = slice(tail_at, tail_at + 32)
            nodal[at_rows] = jnp.where(lane == 2 * p + at, total, nodal[at_rows])

    def whole_product(p, squares):
        result = acc[p] + jnp.dot(ghost[...], edge_weights[p], preferred_element_type=F32)
        for at in range(2):
            s = 2 * p + at
            mine = result[:, at * count : (at + 1) * count]
            cols_ref[pl.ds(s, modes, stride=snaps), :] = mine
            norm = jnp.sum(mine * mine, axis=0, keepdims=True)
            squares = jnp.where(row == s, norm, squares)
        return squares

    def each_pair(body):
        if pairs <= 4:
            for p in range(pairs):
                body(p)
        else:
            lax.fori_loop(0, pairs, lambda p, c: (body(p), c)[1], 0)

    others = disp.at[pl.ds(0, params - 1), own_part]
    wait_bytes(others, recv_n)
    each_pair(own_product)
    each_pair(own_sums)

    def flipped(ref):
        return jnp.concatenate(
            [jnp.transpose(ref[t * 128 : (t + 1) * 128])[:snaps] for t in range(ref.shape[0] // 128)],
            axis=1,
        )

    part_p[me_p, :, :wide] = flipped(part)
    wait_bytes(backs, recv_d)

    @pl.when(leading)
    def _():
        for c in range(CHUNKS):
            ghost_copy(c).wait_recv()
            for p in range(params - 1):
                hand_on(p, c).start()

    each_pair(edge_forces)
    part_p[me_p, :, wide:] = flipped(nodal)

    def to_lead():
        return remote(part_p.at[me_p], part_p.at[me_p], send_p, recv_p, dev(me_e, lead))

    @pl.when(jnp.logical_not(leading))
    def _():
        to_lead().start()

    @pl.when(jnp.logical_not(leading))
    def _():
        wait_bytes(ghost_in, recv_f)

    if ghosts % 128 == 0:
        ghost[:, :tail_at] = ghost_in[:modes]
    else:
        ghost[:, : 2 * ghosts] = ghost_in[:modes]
        ghost[:half, 2 * ghosts : tail_at] = ghost_in[rows - half :, :ghosts]
        ghost[half:, 2 * ghosts : tail_at] = ghost_in[rows - half : rows - 2 * half + modes, ghosts:]
    def to_elem(j):
        to = me_e + (j + 1)
        to = jnp.where(to >= elems, to - elems, to)
        return remote(part_e.at[me_e], part_e.at[me_e], send_e, recv_e, dev(to, lead))

    every_elem = part_e.at[pl.ds(0, elems - 1)]

    def result(p):
        return remote(total_ref, total_ref, send_t.at[p], recv_t, dev(me_e, p))

    row = lax.broadcasted_iota(jnp.int32, (snaps, 128), 0)
    across = lax.broadcasted_iota(jnp.int32, (snaps, 128), 1)
    squares = jnp.zeros((snaps, count), F32)
    if pairs <= 4:
        for p in range(pairs):
            squares = whole_product(p, squares)
    else:
        squares = lax.fori_loop(0, pairs, whole_product, squares)

    norm = jnp.sum(jnp.sqrt(squares), axis=1, keepdims=True)
    norms[me] = jnp.sum(jnp.where(row == across, norm, 0.0), axis=0, keepdims=True)

    @pl.when(jnp.logical_not(climbing & top))
    def _():
        pl.semaphore_wait(known, 1)

    def norm_copy(j):
        return remote(norms.at[me], norms.at[me], send_c, recv_c, other(j))

    repeat(devices - 1, lambda j: norm_copy(j).start())

    @pl.when(leading)
    def _():
        wait_bytes(part_p.at[pl.ds(0, params - 1)], recv_p)
        chip = part_p[0]
        for p in range(1, params):
            chip = chip + part_p[p]
        force = chip[:, wide:]
        force0 = force.astype(BF16)
        left = force - force0.astype(F32)
        force1 = left.astype(BF16)
        force2 = (left - force1.astype(F32)).astype(BF16)
        both = (((1,), (1,)), ((), ()))
        total = lax.dot_general(force2, ghost[...], both, preferred_element_type=F32)
        total = total + lax.dot_general(force1, ghost[...], both, preferred_element_type=F32)
        total = total + lax.dot_general(force0, ghost[...], both, preferred_element_type=F32)
        part_e[me_e] = chip[:, :wide]
        part_e[me_e, :, :modes] = chip[:, :modes] + total
        repeat(elems - 1, lambda j: to_elem(j).start())
        wait_bytes(every_elem, recv_e)
        total = part_e[0]
        for e in range(1, elems):
            total = total + part_e[e]
        total_ref[...] = total
        for p in range(params - 1):
            result(p).start()

    everyone = norms.at[pl.ds(0, devices - 1)]
    wait_bytes(everyone, recv_c)
    whole = norms[0]
    for d in range(1, devices):
        whole = whole + norms[d]
    diagonal = jnp.where(row == across, jnp.broadcast_to(whole, (snaps, 128)), 0.0)
    row_scale = jnp.sum(diagonal, axis=1, keepdims=True) / elem_total
    inverse_ref[...] = jnp.broadcast_to(1.0 / row_scale, (snaps, count))

    @pl.when(jnp.logical_not(leading))
    def _():
        result(0).wait_recv()

    target_ref[...] = total_ref[:, :modes] / (row_scale * math.sqrt(elem_total))

    wait_bytes(others, send_n)
    wait_bytes(everyone, send_c)

    @pl.when(first)
    def _():
        to_relay().wait_send()

    @pl.when(jnp.logical_not(first))
    def _():
        wait_bytes(backs, send_d)

    @pl.when(relaying)
    def _():
        for q in range(params):
            wait_bytes(relay_disp, send_rd.at[q])
        wait_bytes(relay_ghost, send_rg)

    @pl.when(leading)
    def _():
        wait_bytes(packed, send_g)
        for p in range(params - 1):
            wait_bytes(ghost_in, send_f.at[p])
        wait_bytes(every_elem, send_e)
        for p in range(params - 1):
            result(p).wait_send()

    @pl.when(jnp.logical_not(leading))
    def _():
        to_lead().wait_send()


def finish_kernel(cols_ref, inverse_ref, target_ref, training_hbm, target_hbm, training, sem):
    modes, snaps, count = training.shape
    copies = [pltpu.make_async_copy(target_ref, target_hbm, sem.at[0])]
    copies[0].start()
    inverse = inverse_ref[...][None]
    chunks = sem.shape[0] - 1
    size = modes // chunks
    for c in range(chunks):
        rows = pl.ds(c * size, size)
        piece = cols_ref[c * size * snaps : (c + 1) * size * snaps]
        training[rows] = (piece.reshape(size, snaps, count) * inverse).astype(BF16)
        copies.append(pltpu.make_async_copy(training.at[rows], training_hbm.at[rows], sem.at[c + 1]))
        copies[-1].start()
    for copy in copies:
        copy.wait()


def local(elems, params, coords, basis_rows, connectivity, modulus, stiffness):
    own_snaps, modes = coords.shape
    nodes = basis_rows.shape[2]
    count = connectivity.shape[0]
    snaps = own_snaps * params
    ghosts = nodes // 4
    if ghosts % 128 == 0:
        packed = (round_up(modes, 16), 3 * ghosts)
    else:
        packed = (round_up(modes, 16) + round_up(-(-modes // 2), 16), 2 * ghosts)
    edge = round_up(3 * ghosts + 32, 128)
    tiles = nodes // 128 + -(-ghosts // 128)
    wide = round_up(modes, 128)
    dofs = stiffness.shape[0]
    devices = elems * params
    inner = 4
    pairs = snaps // 2
    dma = pltpu.SemaphoreType.DMA
    vmem = pl.BlockSpec(memory_space=pltpu.VMEM)
    hbm = pl.BlockSpec(memory_space=pltpu.HBM)
    cols, inverse, target = pl.pallas_call(
        functools.partial(kernel, elems, params, inner),
        out_shape=(
            jax.ShapeDtypeStruct((modes * snaps, count), F32),
            jax.ShapeDtypeStruct((snaps, count), F32),
            jax.ShapeDtypeStruct((snaps, modes), F32),
        ),
        in_specs=[hbm] * 5,
        out_specs=(vmem, vmem, vmem),
        scratch_shapes=[
            pltpu.VMEM((own_snaps, modes), BF16),
            pltpu.VMEM((3, modes, nodes), BF16),
            pltpu.VMEM((8, count), jnp.int32),
            pltpu.VMEM((1, count), F32),
            pltpu.VMEM((dofs, dofs), F32),
            pltpu.VMEM(packed, BF16),
            pltpu.VMEM(packed, BF16),
            pltpu.VMEM((modes, edge), BF16),
            pltpu.VMEM((params, tiles, 3, own_snaps, 128), F32),
            pltpu.VMEM((pairs, dofs, 2 * count), F32),
            pltpu.VMEM((pairs if pairs <= 4 else 1, 3 * nodes, 2 * count), BF16),
            pltpu.VMEM((pairs, edge, 2 * count), BF16),
            pltpu.VMEM((pairs, modes, 2 * count), F32),
            pltpu.VMEM((wide, 128), F32),
            pltpu.VMEM((edge, 128), F32),
            pltpu.VMEM((devices, 1, 128), F32),
            pltpu.VMEM((params, snaps, wide + edge), F32),
            pltpu.VMEM((elems, snaps, wide), F32),
            pltpu.VMEM((snaps, wide), F32),
            pltpu.VMEM((params, tiles - nodes // 128, 3, own_snaps, 128), F32),
            pltpu.VMEM(packed, BF16),
            dma((4,)), dma, dma, dma((CHUNKS,)), dma, dma, dma((params - 1,)), dma,
            dma, dma, dma, dma((params - 1,)), dma,
            dma((params,)), dma, dma, dma((CHUNKS,)),
            pltpu.SemaphoreType.REGULAR, pltpu.SemaphoreType.REGULAR,
        ],
        compiler_params=pltpu.CompilerParams(
            collective_id=0, has_side_effects=True, vmem_limit_bytes=40 * 1024 * 1024
        ),
    )(*(pltpu.with_memory_space_constraint(x, pltpu.HBM) for x in (
        coords, basis_rows, connectivity.T, modulus[None], stiffness
    )))
    chunks = next(c for c in (4, 3, 2, 1) if modes % c == 0)
    training, target = pl.pallas_call(
        finish_kernel,
        out_shape=(
            jax.ShapeDtypeStruct((modes, snaps, count), BF16),
            jax.ShapeDtypeStruct((snaps, modes), F32),
        ),
        in_specs=[vmem, vmem, vmem],
        out_specs=(hbm, hbm),
        scratch_shapes=[pltpu.VMEM((modes, snaps, count), BF16), dma((chunks + 1,))],
        compiler_params=pltpu.CompilerParams(vmem_limit_bytes=20 * 1024 * 1024),
    )(cols, inverse, target)
    return (jnp.transpose(training, (1, 0, 2)), target)


def solution(mesh):
    in_specs = (
        P("param", None),
        P(None, None, "elem"),
        P(("elem", "param"), None),
        P(("elem", "param")),
        P(),
    )
    out_specs = (P(None, None, ("elem", "param")), P())
    run = functools.partial(local, mesh.shape["elem"], mesh.shape["param"])
    return jax.shard_map(run, mesh=mesh, in_specs=in_specs, out_specs=out_specs, check_vma=False)
```

```python
import functools
import math

import jax
import jax.numpy as jnp
from jax import lax
from jax.experimental import pallas as pl
from jax.experimental.pallas import tpu as pltpu
from jax.sharding import PartitionSpec as P

LOGICAL = pl.DeviceIdType.LOGICAL
F32 = jnp.float32
BF16 = jnp.bfloat16
UNROLL = 64
CHUNKS = 4


def round_up(value, to):
    return -(-value // to) * to


def repeat(count, body):
    if count <= UNROLL:
        for j in range(count):
            body(j)
    else:
        lax.fori_loop(0, count, lambda j, c: (body(j), c)[1], 0)


def kernel(
    elems, params, inner,
    coords_hbm, basis_hbm, conn_hbm, modulus_hbm, stiff_hbm,
    cols_ref, inverse_ref, target_ref,
    coords_ref, basis_ref, conn_ref, modulus_ref, stiff_ref,
    packed, ghost_in, ghost, disp, corner_disp, weights, edge_weights, acc, part, nodal,
    norms, part_p, part_e, total_ref, relay_disp, relay_ghost,
    load, load_b, send_g, recv_g, recv_d, recv_n, send_f, recv_f,
    recv_c, recv_p, recv_e, send_t, recv_t,
    send_rd, recv_rd, send_rg, recv_rg, climb, known,
):
    send_d, send_n, send_p, send_e = [load.at[i] for i in range(4)]
    send_c = load_b
    own_snaps, modes = coords_hbm.shape
    dofs = stiff_hbm.shape[0]
    snaps = own_snaps * params
    pairs = snaps // 2
    nodes = basis_hbm.shape[2]
    ghosts = nodes // 4
    count = conn_hbm.shape[1]
    devices = elems * params
    outer = elems // inner
    elem_total = count * devices
    wide, edge = part_e.shape[2], ghost.shape[1]
    own_tiles = nodes // 128
    ghost_tiles = disp.shape[1] - own_tiles
    me_e, me_p = lax.axis_index("elem"), lax.axis_index("param")
    me = me_e * params + me_p
    lead = params - 1
    leading = me_p == lead
    first, last = me_e == 0, me_e == elems - 1
    before = jnp.where(first, elems - 1, me_e - 1)
    relay = (elems // 4 + 2) * params + lead
    relaying = me == relay
    me_o, me_i = lax.div(me_e, inner), lax.rem(me_e, inner)
    bottom, top = me_o == 0, me_o == outer - 1
    guide = inner // 2
    climbing = (me_p == 0) & (me_i == guide)

    def dev(e, p):
        return e * params + p

    def other(j):
        to = me + (j + 1)
        return jnp.where(to >= devices, to - devices, to)

    def signal(semaphore, device):
        pl.semaphore_signal(semaphore, inc=1, device_id=device, device_id_type=LOGICAL)

    def remote(src, dst, send, recv, device):
        return pltpu.make_async_remote_copy(
            src_ref=src, dst_ref=dst, send_sem=send, recv_sem=recv,
            device_id=device, device_id_type=LOGICAL,
        )

    def wait_bytes(ref, semaphore):
        pltpu.make_async_copy(ref, ref, semaphore).wait()

    load_basis = pltpu.make_async_copy(basis_hbm, basis_ref, load_b)
    smalls = [
        pltpu.make_async_copy(src, dst, load.at[i])
        for i, (src, dst) in enumerate([
            (coords_hbm, coords_ref), (conn_hbm, conn_ref),
            (modulus_hbm, modulus_ref), (stiff_hbm, stiff_ref),
        ])
    ]
    for copy in [load_basis] + smalls:
        copy.start()

    barrier = pltpu.get_barrier_semaphore()
    @pl.when(first | last)
    def _():
        signal(barrier, relay)

    @pl.when(relaying)
    def _():
        for p in range(params):
            signal(barrier, dev(elems - 1, p))
            signal(barrier, dev(0, p))

    @pl.when(jnp.logical_not(first))
    def _():
        for p in range(params):
            signal(barrier, dev(me_e - 1, p))

    @pl.when(jnp.logical_not(last))
    def _():
        for p in range(params):
            signal(barrier, dev(me_e + 1, p))

    @pl.when(climbing & jnp.logical_not(bottom))
    def _():
        signal(barrier, dev(me_e - inner, 0))

    @pl.when(climbing & jnp.logical_not(top))
    def _():
        signal(barrier, dev(me_e + inner, 0))

    for j in range(1, params):
        to = me_p + j
        signal(barrier, dev(me_e, jnp.where(to >= params, to - params, to)))

    @pl.when(me_i != guide)
    def _():
        signal(barrier, dev(me_o * inner + guide, 0))

    greeted = params - 1 + jnp.where(first | last, 1, params) + params
    greeted += jnp.where(relaying, 2 * params, 0)
    climbs = (inner - 1) * params + 2 - jnp.where(bottom | top, 1, 0)
    greeted += jnp.where(climbing, climbs, 0)

    part[...] = jnp.zeros_like(part)
    nodal[...] = jnp.zeros_like(nodal)
    tail_at = 3 * ghosts
    for p in range(pairs):
        edge_weights[p, tail_at:] = jnp.zeros((edge - tail_at, 2 * count), BF16)
    for copy in smalls:
        copy.wait()
    coords = coords_ref[...]
    load_basis.wait()
    for k in range(3):
        moved = jnp.dot(coords, basis_ref[k], preferred_element_type=F32)
        moved = moved.astype(BF16).astype(F32)
        for t in range(own_tiles):
            disp[me_p, t, k] = moved[:, t * 128 : (t + 1) * 128]
    rows = packed.shape[0]
    if ghosts % 128 == 0:
        for k in range(3):
            packed[:modes, k * ghosts : (k + 1) * ghosts] = basis_ref[k, :, :ghosts]
    else:
        half = rows - round_up(modes, 16)
        packed[:modes, :ghosts] = basis_ref[0, :, :ghosts]
        packed[:modes, ghosts:] = basis_ref[1, :, :ghosts]
        packed[rows - half :, :ghosts] = basis_ref[2, :half, :ghosts]
        packed[rows - half : rows - 2 * half + modes, ghosts:] = basis_ref[2, half:, :ghosts]

    pl.semaphore_wait(barrier, greeted)
    own_part, ghost_part = pl.ds(0, own_tiles), pl.ds(own_tiles, ghost_tiles)
    front = disp.at[me_p, pl.ds(0, ghost_tiles)]
    backs = disp.at[:, ghost_part]

    def ghost_disp(p):
        turn = lax.rem(me_p + p, params)
        return remote(front, disp.at[me_p, ghost_part], send_d, recv_d, dev(before, turn))

    def own_disp(p):
        turn = lax.rem(me_p + p, params)
        mine = disp.at[me_p, own_part]
        return remote(mine, mine, send_n, recv_n, dev(me_e, turn))

    def to_relay():
        return remote(front, relay_disp.at[me_p], send_d, recv_rd, relay)

    def from_relay(p):
        return remote(relay_disp, backs, send_rd.at[p], recv_d, dev(elems - 1, p))

    cuts = [rows // 16 * c // CHUNKS * 16 for c in range(CHUNKS + 1)]

    def cut(ref, c):
        return ref.at[pl.ds(cuts[c], cuts[c + 1] - cuts[c])]

    def ghost_copy(c):
        return remote(cut(packed, c), cut(ghost_in, c), send_g, recv_g.at[c], dev(before, lead))

    def ghost_to_relay(c):
        return remote(cut(packed, c), cut(relay_ghost, c), send_g, recv_rg.at[c], relay)

    def ghost_from_relay(c):
        return remote(
            cut(relay_ghost, c), cut(ghost_in, c), send_rg, recv_g.at[c], dev(elems - 1, lead)
        )

    def hand_on(p, c):
        return remote(cut(ghost_in, c), cut(ghost_in, c), send_f.at[p], recv_f, dev(me_e, p))

    @pl.when(first)
    def _():
        to_relay().start()

    @pl.when(jnp.logical_not(first))
    def _():
        for p in range(params):
            ghost_disp(p).start()

    @pl.when(first & leading)
    def _():
        for c in range(CHUNKS):
            ghost_to_relay(c).start()

    @pl.when(jnp.logical_not(first | relaying) & leading)
    def _():
        for c in range(CHUNKS):
            ghost_copy(c).start()

    for p in range(1, params):
        own_disp(p).start()

    @pl.when(relaying)
    def _():
        wait_bytes(relay_disp, recv_rd)
        for p in range(params):
            from_relay(p).start()
        for c in range(CHUNKS):
            ghost_to_relay(c).wait_recv()
            ghost_from_relay(c).start()
        for c in range(CHUNKS):
            ghost_copy(c).start()

    @pl.when(climbing & jnp.logical_not(bottom))
    def _():
        pl.semaphore_wait(climb, 1)

    @pl.when(climbing & jnp.logical_not(top))
    def _():
        signal(climb, dev(me_e + inner, 0))

    @pl.when(climbing & top)
    def _():
        repeat(devices - 1, lambda j: signal(known, other(j)))

    corners = conn_ref[...]
    base = jnp.min(corners, axis=0, keepdims=True)
    residue = corners % 8
    lane_at = corners % 128
    tile_at = corners // 128
    row8 = lax.broadcasted_iota(jnp.int32, (8, count), 0)
    lane = lax.broadcasted_iota(jnp.int32, (1, 128), 1)
    hits = [residue[a : a + 1] == row8 for a in range(8)]

    def inside(start, height):
        node = start + lax.broadcasted_iota(jnp.int32, (height, count), 0)
        return (node >= base) & (node < base + 8)

    own_rows = lax.broadcasted_iota(jnp.int32, (nodes, count), 0) < nodes - 8
    own_mask = jnp.where(inside(0, nodes) & own_rows, 1.0, 0.0).astype(BF16)
    ghost_mask = jnp.where(inside(nodes, ghosts), 1.0, 0.0)
    tail_mask = jnp.where(inside(nodes - 8, 8), 1.0, 0.0)
    stiff = stiff_ref[...]
    high = stiff.astype(BF16)
    rest = stiff - high.astype(F32)
    mid = rest.astype(BF16)
    low = (rest - mid.astype(F32)).astype(BF16)
    modulus = modulus_ref[...]
    modulus2 = jnp.concatenate([modulus, modulus], axis=1)
    tails = [basis_ref[k, :, nodes - 8 :] for k in range(3)]
    start = tail_at // 128 * 128
    blank = [jnp.zeros((modes, tail_at - start), BF16)] if tail_at > start else []
    after = [jnp.zeros((modes, edge - tail_at - 24), BF16)]
    ghost[:, start:] = jnp.concatenate(blank + tails + after, axis=1)

    def gathered(p, found, tiles):
        pieces = []
        for at in range(2):
            s = 2 * p + at
            parts = []
            for k in range(3):
                piece = found[k * 8 : (k + 1) * 8, at * count : (at + 1) * count]
                for t in tiles:
                    line = disp[s // own_snaps, t, k, pl.ds(s % own_snaps, 1), :]
                    got = jnp.take_along_axis(jnp.broadcast_to(line, (8, 128)), lane_at, axis=1)
                    piece = jnp.where(tile_at == t, got, piece)
                parts.append(piece)
            pieces.append(jnp.concatenate(parts, axis=0))
        return jnp.concatenate(pieces, axis=1)

    def forces_of(moved):
        moved16 = moved.astype(BF16)
        linear = jnp.dot(low, moved16, preferred_element_type=F32)
        linear = linear + jnp.dot(mid, moved16, preferred_element_type=F32)
        linear = linear + jnp.dot(high, moved16, preferred_element_type=F32)
        return (modulus2 * (linear + 0.25 * moved * moved * moved)).astype(BF16).astype(F32)

    def spread_of(forces, at, k):
        spread = jnp.zeros((8, count), F32)
        for a in range(8):
            force = forces[k * 8 + a : k * 8 + a + 1, at * count : (at + 1) * count]
            spread = spread + jnp.where(hits[a], force, 0.0)
        return spread.astype(BF16).astype(F32)

    def own_product(p):
        slot = p if weights.shape[0] > 1 else 0
        moved = gathered(p, jnp.zeros((dofs, 2 * count), F32), range(own_tiles))
        corner_disp[p] = moved
        forces = forces_of(moved)
        for at in range(2):
            columns = slice(at * count, (at + 1) * count)
            for k in range(3):
                spread = spread_of(forces, at, k)
                twice = jnp.concatenate([spread, spread], axis=0).astype(BF16)
                tall = jnp.concatenate([twice] * (nodes // 16), axis=0) * own_mask
                weights[slot, k * nodes : (k + 1) * nodes, columns] = tall
        total = jnp.dot(basis_ref[0], weights[slot, :nodes], preferred_element_type=F32)
        for k in range(1, 3):
            total = total + jnp.dot(
                basis_ref[k], weights[slot, k * nodes : (k + 1) * nodes], preferred_element_type=F32
            )
        acc[p] = total

    def own_sums(p):
        for at in range(2):
            mine = acc[p, :, at * count : (at + 1) * count]
            total = jnp.sum(mine, axis=1, keepdims=True)
            part[:modes] = jnp.where(lane == 2 * p + at, total, part[:modes])

    def edge_forces(p):
        moved = gathered(p, corner_disp[p], range(own_tiles, own_tiles + ghost_tiles))
        forces = forces_of(moved)
        for at in range(2):
            columns = slice(at * count, (at + 1) * count)
            ends = []
            for k in range(3):
                spread = spread_of(forces, at, k)
                tall = jnp.concatenate([spread] * (ghosts // 8), axis=0) * ghost_mask
                edge_weights[p, k * ghosts : (k + 1) * ghosts, columns] = tall.astype(BF16)
                ends.append(spread * tail_mask)
                total = jnp.sum(tall, axis=1, keepdims=True)
                at_rows = slice(k * ghosts, (k + 1) * ghosts)
                nodal[at_rows] = jnp.where(lane == 2 * p + at, total, nodal[at_rows])
            end = jnp.concatenate(ends + [jnp.zeros((8, count), F32)], axis=0)
            edge_weights[p, tail_at : tail_at + 32, columns] = end.astype(BF16)
            total = jnp.sum(end, axis=1, keepdims=True)
            at_rows = slice(tail_at, tail_at + 32)
            nodal[at_rows] = jnp.where(lane == 2 * p + at, total, nodal[at_rows])

    def whole_product(p, squares):
        result = acc[p] + jnp.dot(ghost[...], edge_weights[p], preferred_element_type=F32)
        for at in range(2):
            s = 2 * p + at
            mine = result[:, at * count : (at + 1) * count]
            cols_ref[pl.ds(s, modes, stride=snaps), :] = mine
            norm = jnp.sum(mine * mine, axis=0, keepdims=True)
            squares = jnp.where(row == s, norm, squares)
        return squares

    def each_pair(body):
        if pairs <= 4:
            for p in range(pairs):
                body(p)
        else:
            lax.fori_loop(0, pairs, lambda p, c: (body(p), c)[1], 0)

    others = disp.at[pl.ds(0, params - 1), own_part]
    wait_bytes(others, recv_n)
    each_pair(own_product)
    each_pair(own_sums)

    def flipped(ref):
        return jnp.concatenate(
            [jnp.transpose(ref[t * 128 : (t + 1) * 128])[:snaps] for t in range(ref.shape[0] // 128)],
            axis=1,
        )

    part_p[me_p, :, :wide] = flipped(part)
    wait_bytes(backs, recv_d)

    @pl.when(leading)
    def _():
        for c in range(CHUNKS):
            ghost_copy(c).wait_recv()
            for p in range(params - 1):
                hand_on(p, c).start()

    each_pair(edge_forces)
    part_p[me_p, :, wide:] = flipped(nodal)

    def to_lead():
        return remote(part_p.at[me_p], part_p.at[me_p], send_p, recv_p, dev(me_e, lead))

    @pl.when(jnp.logical_not(leading))
    def _():
        to_lead().start()

    @pl.when(jnp.logical_not(leading))
    def _():
        wait_bytes(ghost_in, recv_f)

    if ghosts % 128 == 0:
        ghost[:, :tail_at] = ghost_in[:modes]
    else:
        ghost[:, : 2 * ghosts] = ghost_in[:modes]
        ghost[:half, 2 * ghosts : tail_at] = ghost_in[rows - half :, :ghosts]
        ghost[half:, 2 * ghosts : tail_at] = ghost_in[rows - half : rows - 2 * half + modes, ghosts:]
    def to_elem(j):
        to = me_e + (j + 1)
        to = jnp.where(to >= elems, to - elems, to)
        return remote(part_e.at[me_e], part_e.at[me_e], send_e, recv_e, dev(to, lead))

    every_elem = part_e.at[pl.ds(0, elems - 1)]

    def result(p):
        return remote(total_ref, total_ref, send_t.at[p], recv_t, dev(me_e, p))

    row = lax.broadcasted_iota(jnp.int32, (snaps, 128), 0)
    across = lax.broadcasted_iota(jnp.int32, (snaps, 128), 1)

    def finish_norm():
        squares = jnp.zeros((snaps, count), F32)
        if pairs <= 4:
            for p in range(pairs):
                squares = whole_product(p, squares)
        else:
            squares = lax.fori_loop(0, pairs, whole_product, squares)
        norm = jnp.sum(jnp.sqrt(squares), axis=1, keepdims=True)
        norms[me] = jnp.sum(jnp.where(row == across, norm, 0.0), axis=0, keepdims=True)

    @pl.when(jnp.logical_not(leading))
    def _():
        finish_norm()

    @pl.when(leading)
    def _():
        wait_bytes(part_p.at[pl.ds(0, params - 1)], recv_p)
        finish_norm()
        chip = part_p[0]
        for p in range(1, params):
            chip = chip + part_p[p]
        force = chip[:, wide:]
        high = force.astype(BF16).astype(F32)
        left = force - high
        mid = left.astype(BF16).astype(F32)
        forces = jnp.concatenate([left - mid, mid, high], axis=0).astype(BF16)
        both = (((1,), (1,)), ((), ()))
        parts = lax.dot_general(forces, ghost[...], both, preferred_element_type=F32)
        total = parts[:snaps] + parts[snaps : 2 * snaps] + parts[2 * snaps :]
        part_e[me_e] = chip[:, :wide]
        part_e[me_e, :, :modes] = chip[:, :modes] + total

    @pl.when(jnp.logical_not(climbing & top))
    def _():
        pl.semaphore_wait(known, 1)

    def norm_copy(j):
        return remote(norms.at[me], norms.at[me], send_c, recv_c, other(j))

    repeat(devices - 1, lambda j: norm_copy(j).start())

    @pl.when(leading)
    def _():
        repeat(elems - 1, lambda j: to_elem(j).start())
        wait_bytes(every_elem, recv_e)
        total = part_e[0]
        for e in range(1, elems):
            total = total + part_e[e]
        total_ref[...] = total
        for p in range(params - 1):
            result(p).start()

    everyone = norms.at[pl.ds(0, devices - 1)]
    wait_bytes(everyone, recv_c)
    whole = norms[0]
    for d in range(1, devices):
        whole = whole + norms[d]
    diagonal = jnp.where(row == across, jnp.broadcast_to(whole, (snaps, 128)), 0.0)
    row_scale = jnp.sum(diagonal, axis=1, keepdims=True) / elem_total
    inverse_ref[...] = jnp.broadcast_to(1.0 / row_scale, (snaps, count))

    @pl.when(jnp.logical_not(leading))
    def _():
        result(0).wait_recv()

    target_ref[...] = total_ref[:, :modes] / (row_scale * math.sqrt(elem_total))

    wait_bytes(others, send_n)
    wait_bytes(everyone, send_c)

    @pl.when(first)
    def _():
        to_relay().wait_send()

    @pl.when(jnp.logical_not(first))
    def _():
        wait_bytes(backs, send_d)

    @pl.when(relaying)
    def _():
        for p in range(params):
            wait_bytes(relay_disp, send_rd.at[p])
        wait_bytes(relay_ghost, send_rg)

    @pl.when(leading)
    def _():
        wait_bytes(packed, send_g)
        for p in range(params - 1):
            wait_bytes(ghost_in, send_f.at[p])
        wait_bytes(every_elem, send_e)
        for p in range(params - 1):
            result(p).wait_send()

    @pl.when(jnp.logical_not(leading))
    def _():
        to_lead().wait_send()


def finish_kernel(cols_ref, inverse_ref, target_ref, training_hbm, target_hbm, training, sem):
    modes, snaps, count = training.shape
    copies = [pltpu.make_async_copy(target_ref, target_hbm, sem.at[0])]
    copies[0].start()
    inverse = inverse_ref[...][None]
    chunks = sem.shape[0] - 1
    size = modes // chunks
    for c in range(chunks):
        rows = pl.ds(c * size, size)
        piece = cols_ref[c * size * snaps : (c + 1) * size * snaps]
        training[rows] = (piece.reshape(size, snaps, count) * inverse).astype(BF16)
        copies.append(pltpu.make_async_copy(training.at[rows], training_hbm.at[rows], sem.at[c + 1]))
        copies[-1].start()
    for copy in copies:
        copy.wait()


def local(elems, params, coords, basis_rows, connectivity, modulus, stiffness):
    own_snaps, modes = coords.shape
    nodes = basis_rows.shape[2]
    count = connectivity.shape[0]
    snaps = own_snaps * params
    ghosts = nodes // 4
    if ghosts % 128 == 0:
        packed = (round_up(modes, 16), 3 * ghosts)
    else:
        packed = (round_up(modes, 16) + round_up(-(-modes // 2), 16), 2 * ghosts)
    edge = round_up(3 * ghosts + 32, 128)
    tiles = nodes // 128 + -(-ghosts // 128)
    wide = round_up(modes, 128)
    dofs = stiffness.shape[0]
    devices = elems * params
    inner = 4
    pairs = snaps // 2
    dma = pltpu.SemaphoreType.DMA
    vmem = pl.BlockSpec(memory_space=pltpu.VMEM)
    hbm = pl.BlockSpec(memory_space=pltpu.HBM)
    cols, inverse, target = pl.pallas_call(
        functools.partial(kernel, elems, params, inner),
        out_shape=(
            jax.ShapeDtypeStruct((modes * snaps, count), F32),
            jax.ShapeDtypeStruct((snaps, count), F32),
            jax.ShapeDtypeStruct((snaps, modes), F32),
        ),
        in_specs=[hbm] * 5,
        out_specs=(vmem, vmem, vmem),
        scratch_shapes=[
            pltpu.VMEM((own_snaps, modes), BF16),
            pltpu.VMEM((3, modes, nodes), BF16),
            pltpu.VMEM((8, count), jnp.int32),
            pltpu.VMEM((1, count), F32),
            pltpu.VMEM((dofs, dofs), F32),
            pltpu.VMEM(packed, BF16),
            pltpu.VMEM(packed, BF16),
            pltpu.VMEM((modes, edge), BF16),
            pltpu.VMEM((params, tiles, 3, own_snaps, 128), F32),
            pltpu.VMEM((pairs, dofs, 2 * count), F32),
            pltpu.VMEM((pairs if pairs <= 4 else 1, 3 * nodes, 2 * count), BF16),
            pltpu.VMEM((pairs, edge, 2 * count), BF16),
            pltpu.VMEM((pairs, modes, 2 * count), F32),
            pltpu.VMEM((wide, 128), F32),
            pltpu.VMEM((edge, 128), F32),
            pltpu.VMEM((devices, 1, 128), F32),
            pltpu.VMEM((params, snaps, wide + edge), F32),
            pltpu.VMEM((elems, snaps, wide), F32),
            pltpu.VMEM((snaps, wide), F32),
            pltpu.VMEM((params, tiles - nodes // 128, 3, own_snaps, 128), F32),
            pltpu.VMEM(packed, BF16),
            dma((4,)), dma, dma, dma((CHUNKS,)), dma, dma, dma((params - 1,)), dma,
            dma, dma, dma, dma((params - 1,)), dma,
            dma((params,)), dma, dma, dma((CHUNKS,)),
            pltpu.SemaphoreType.REGULAR, pltpu.SemaphoreType.REGULAR,
        ],
        compiler_params=pltpu.CompilerParams(
            collective_id=0, has_side_effects=True, vmem_limit_bytes=40 * 1024 * 1024
        ),
    )(*(pltpu.with_memory_space_constraint(x, pltpu.HBM) for x in (
        coords, basis_rows, connectivity.T, modulus[None], stiffness
    )))
    chunks = next(c for c in (4, 3, 2, 1) if modes % c == 0)
    training, target = pl.pallas_call(
        finish_kernel,
        out_shape=(
            jax.ShapeDtypeStruct((modes, snaps, count), BF16),
            jax.ShapeDtypeStruct((snaps, modes), F32),
        ),
        in_specs=[vmem, vmem, vmem],
        out_specs=(hbm, hbm),
        scratch_shapes=[pltpu.VMEM((modes, snaps, count), BF16), dma((chunks + 1,))],
        compiler_params=pltpu.CompilerParams(vmem_limit_bytes=20 * 1024 * 1024),
    )(cols, inverse, target)
    return (jnp.transpose(training, (1, 0, 2)), target)


def solution(mesh):
    in_specs = (
        P("param", None),
        P(None, None, "elem"),
        P(("elem", "param"), None),
        P(("elem", "param")),
        P(),
    )
    out_specs = (P(None, None, ("elem", "param")), P())
    run = functools.partial(local, mesh.shape["elem"], mesh.shape["param"])
    return jax.shard_map(run, mesh=mesh, in_specs=in_specs, out_specs=out_specs, check_vma=False)
```

```python
import functools
import math

import jax
import jax.numpy as jnp
from jax import lax
from jax.experimental import pallas as pl
from jax.experimental.pallas import tpu as pltpu
from jax.sharding import PartitionSpec as P

LOGICAL = pl.DeviceIdType.LOGICAL
F32 = jnp.float32
BF16 = jnp.bfloat16
UNROLL = 64
CHUNKS = 5
FAR = 2


def round_up(value, to):
    return -(-value // to) * to


def repeat(count, body):
    if count <= UNROLL:
        for j in range(count):
            body(j)
    else:
        lax.fori_loop(0, count, lambda j, c: (body(j), c)[1], 0)


def kernel(
    elems, params, inner,
    coords_hbm, basis_hbm, conn_hbm, modulus_hbm, stiff_hbm,
    cols_ref, inverse_ref, target_ref,
    coords_ref, basis_ref, conn_ref, modulus_ref, stiff_ref,
    packed, ghost_in, ghost, disp, corner_disp, weights, edge_weights, acc, part, nodal,
    norms, part_p, part_e, total_ref, relay_disp, relay_ghost,
    load, load_b, send_g, recv_g, recv_d, recv_n, send_f, recv_f,
    recv_c, recv_p, recv_e, send_t, recv_t,
    send_rd, recv_rd, send_rg, recv_rg, climb, known,
):
    send_d, send_n, send_p, send_e = [load.at[i] for i in range(4)]
    send_c = load_b
    own_snaps, modes = coords_hbm.shape
    dofs = stiff_hbm.shape[0]
    snaps = own_snaps * params
    pairs = snaps // 2
    nodes = basis_hbm.shape[2]
    ghosts = nodes // 4
    count = conn_hbm.shape[1]
    devices = elems * params
    outer = elems // inner
    elem_total = count * devices
    wide, edge = part_e.shape[2], ghost.shape[1]
    own_tiles = nodes // 128
    ghost_tiles = disp.shape[1] - own_tiles
    me_e, me_p = lax.axis_index("elem"), lax.axis_index("param")
    me = me_e * params + me_p
    lead = params - 1
    leading = me_p == lead
    first, last = me_e == 0, me_e == elems - 1
    before = jnp.where(first, elems - 1, me_e - 1)
    relay = (elems // 4 + 2) * params + lead
    relaying = me == relay
    me_o, me_i = lax.div(me_e, inner), lax.rem(me_e, inner)
    bottom, top = me_o == 0, me_o == outer - 1
    guide = inner // 2
    climbing = (me_p == 0) & (me_i == guide)

    def dev(e, p):
        return e * params + p

    def other(j):
        to = me + (j + 1)
        return jnp.where(to >= devices, to - devices, to)

    def signal(semaphore, device):
        pl.semaphore_signal(semaphore, inc=1, device_id=device, device_id_type=LOGICAL)

    def remote(src, dst, send, recv, device):
        return pltpu.make_async_remote_copy(
            src_ref=src, dst_ref=dst, send_sem=send, recv_sem=recv,
            device_id=device, device_id_type=LOGICAL,
        )

    def wait_bytes(ref, semaphore):
        pltpu.make_async_copy(ref, ref, semaphore).wait()

    load_basis = pltpu.make_async_copy(basis_hbm, basis_ref, load_b)
    smalls = [
        pltpu.make_async_copy(src, dst, load.at[i])
        for i, (src, dst) in enumerate([
            (coords_hbm, coords_ref), (conn_hbm, conn_ref),
            (modulus_hbm, modulus_ref), (stiff_hbm, stiff_ref),
        ])
    ]
    for copy in [load_basis] + smalls:
        copy.start()

    barrier = pltpu.get_barrier_semaphore()
    @pl.when(first | last)
    def _():
        signal(barrier, relay)

    @pl.when(relaying)
    def _():
        for p in range(params):
            signal(barrier, dev(elems - 1, p))
            signal(barrier, dev(0, p))

    @pl.when(jnp.logical_not(first))
    def _():
        for p in range(params):
            signal(barrier, dev(me_e - 1, p))

    @pl.when(jnp.logical_not(last))
    def _():
        for p in range(params):
            signal(barrier, dev(me_e + 1, p))

    @pl.when(climbing & jnp.logical_not(bottom))
    def _():
        signal(barrier, dev(me_e - inner, 0))

    @pl.when(climbing & jnp.logical_not(top))
    def _():
        signal(barrier, dev(me_e + inner, 0))

    for j in range(1, params):
        to = me_p + j
        signal(barrier, dev(me_e, jnp.where(to >= params, to - params, to)))

    @pl.when(me_i != guide)
    def _():
        signal(barrier, dev(me_o * inner + guide, 0))

    greeted = params - 1 + jnp.where(first | last, 1, params) + params
    greeted += jnp.where(relaying, 2 * params, 0)
    climbs = (inner - 1) * params + 2 - jnp.where(bottom | top, 1, 0)
    greeted += jnp.where(climbing, climbs, 0)

    part[...] = jnp.zeros_like(part)
    nodal[...] = jnp.zeros_like(nodal)
    tail_at = 3 * ghosts
    for p in range(pairs):
        edge_weights[p, tail_at:] = jnp.zeros((edge - tail_at, 2 * count), BF16)
    for copy in smalls:
        copy.wait()
    coords = coords_ref[...]
    load_basis.wait()
    for k in range(3):
        moved = jnp.dot(coords, basis_ref[k], preferred_element_type=F32)
        moved = moved.astype(BF16).astype(F32)
        for t in range(own_tiles):
            disp[me_p, t, k] = moved[:, t * 128 : (t + 1) * 128]
    rows, lanes = packed.shape
    a_rows = round_up(modes, 16)
    half = rows - a_rows
    if half:
        packed[:half, :ghosts] = basis_ref[2, :half, :ghosts]
        packed[: modes - half, ghosts:] = basis_ref[2, half:, :ghosts]
    for k in range(lanes // ghosts):
        packed[half : half + modes, k * ghosts : (k + 1) * ghosts] = basis_ref[k, :, :ghosts]

    pl.semaphore_wait(barrier, greeted)
    own_part, ghost_part = pl.ds(0, own_tiles), pl.ds(own_tiles, ghost_tiles)
    front = disp.at[me_p, pl.ds(0, ghost_tiles)]
    backs = disp.at[:, ghost_part]

    def ghost_disp(p):
        turn = lax.rem(me_p + p, params)
        return remote(front, disp.at[me_p, ghost_part], send_d, recv_d, dev(before, turn))

    def own_disp(p):
        turn = lax.rem(me_p + p, params)
        mine = disp.at[me_p, own_part]
        return remote(mine, mine, send_n, recv_n, dev(me_e, turn))

    def to_relay():
        return remote(front, relay_disp.at[me_p], send_d, recv_rd, relay)

    def from_relay(p):
        return remote(relay_disp, backs, send_rd.at[p], recv_d, dev(elems - 1, p))

    fore = 2 if half else 0
    rear = CHUNKS - fore
    cuts = [half // 16 * c // fore * 16 for c in range(fore)]
    cuts += [half + a_rows // 16 * c // rear * 16 for c in range(rear + 1)]

    def cut(ref, c):
        return ref.at[pl.ds(cuts[c], cuts[c + 1] - cuts[c])]

    def ghost_copy(c):
        return remote(cut(packed, c), cut(ghost_in, c), send_g, recv_g.at[c], dev(before, lead))

    def ghost_to_relay(c):
        return remote(cut(packed, c), cut(relay_ghost, c), send_g, recv_rg.at[c], relay)

    def ghost_from_relay(c):
        return remote(
            cut(relay_ghost, c), cut(ghost_in, c), send_rg, recv_g.at[c], dev(elems - 1, lead)
        )

    def hand_on(p, c):
        to = cut(ghost_in, c)
        if c >= fore:
            to = ghost.at[pl.ds(cuts[c] - half, cuts[c + 1] - cuts[c]), pl.ds(0, lanes)]
        kind = 0 if c < fore else 1
        return remote(cut(ghost_in, c), to, send_f.at[p], recv_f.at[kind], dev(me_e, p))

    @pl.when(first)
    def _():
        to_relay().start()

    @pl.when(jnp.logical_not(first))
    def _():
        for p in range(params):
            ghost_disp(p).start()

    @pl.when(first & leading)
    def _():
        for c in range(CHUNKS):
            ghost_to_relay(c).start()

    @pl.when(jnp.logical_not(first | relaying) & leading)
    def _():
        for c in range(CHUNKS):
            ghost_copy(c).start()

    for p in range(1, params):
        own_disp(p).start()

    @pl.when(relaying)
    def _():
        wait_bytes(relay_disp, recv_rd)
        for p in range(params):
            from_relay(p).start()
        for c in range(CHUNKS):
            ghost_to_relay(c).wait_recv()
            ghost_from_relay(c).start()
        for c in range(CHUNKS):
            ghost_copy(c).start()

    @pl.when(climbing & jnp.logical_not(bottom))
    def _():
        pl.semaphore_wait(climb, 1)

    @pl.when(climbing & jnp.logical_not(top))
    def _():
        signal(climb, dev(me_e + inner, 0))

    @pl.when(climbing & top)
    def _():
        repeat(devices - 1, lambda j: signal(known, other(j)))

    corners = conn_ref[...]
    base = jnp.min(corners, axis=0, keepdims=True)
    residue = corners % 8
    lane_at = corners % 128
    tile_at = corners // 128
    row8 = lax.broadcasted_iota(jnp.int32, (8, count), 0)
    lane = lax.broadcasted_iota(jnp.int32, (1, 128), 1)
    hits = [residue[a : a + 1] == row8 for a in range(8)]

    def inside(start, height):
        node = start + lax.broadcasted_iota(jnp.int32, (height, count), 0)
        return (node >= base) & (node < base + 8)

    own_rows = lax.broadcasted_iota(jnp.int32, (nodes, count), 0) < nodes - 8
    own_mask = jnp.where(inside(0, nodes) & own_rows, 1.0, 0.0).astype(BF16)
    ghost_mask = jnp.where(inside(nodes, ghosts), 1.0, 0.0)
    tail_mask = jnp.where(inside(nodes - 8, 8), 1.0, 0.0)
    stiff = stiff_ref[...]
    high = stiff.astype(BF16)
    rest = stiff - high.astype(F32)
    mid = rest.astype(BF16)
    low = (rest - mid.astype(F32)).astype(BF16)
    modulus = modulus_ref[...]
    modulus2 = jnp.concatenate([modulus, modulus], axis=1)
    tails = [basis_ref[k, :, nodes - 8 :] for k in range(3)]
    start = tail_at // 128 * 128
    blank = [jnp.zeros((modes, tail_at - start), BF16)] if tail_at > start else []
    after = [jnp.zeros((modes, edge - tail_at - 24), BF16)]
    ghost[:modes, start:] = jnp.concatenate(blank + tails + after, axis=1)

    def gathered(p, found, tiles):
        pieces = []
        for at in range(2):
            s = 2 * p + at
            parts = []
            for k in range(3):
                piece = found[k * 8 : (k + 1) * 8, at * count : (at + 1) * count]
                for t in tiles:
                    line = disp[s // own_snaps, t, k, pl.ds(s % own_snaps, 1), :]
                    got = jnp.take_along_axis(jnp.broadcast_to(line, (8, 128)), lane_at, axis=1)
                    piece = jnp.where(tile_at == t, got, piece)
                parts.append(piece)
            pieces.append(jnp.concatenate(parts, axis=0))
        return jnp.concatenate(pieces, axis=1)

    def forces_of(moved):
        moved16 = moved.astype(BF16)
        linear = jnp.dot(low, moved16, preferred_element_type=F32)
        linear = linear + jnp.dot(mid, moved16, preferred_element_type=F32)
        linear = linear + jnp.dot(high, moved16, preferred_element_type=F32)
        return (modulus2 * (linear + 0.25 * moved * moved * moved)).astype(BF16).astype(F32)

    def spread_of(forces, at, k):
        spread = jnp.zeros((8, count), F32)
        for a in range(8):
            force = forces[k * 8 + a : k * 8 + a + 1, at * count : (at + 1) * count]
            spread = spread + jnp.where(hits[a], force, 0.0)
        return spread.astype(BF16).astype(F32)

    def own_product(p):
        slot = p if weights.shape[0] > 1 else 0
        moved = gathered(p, jnp.zeros((dofs, 2 * count), F32), range(own_tiles))
        corner_disp[p] = moved
        forces = forces_of(moved)
        for at in range(2):
            columns = slice(at * count, (at + 1) * count)
            for k in range(3):
                spread = spread_of(forces, at, k)
                twice = jnp.concatenate([spread, spread], axis=0).astype(BF16)
                tall = jnp.concatenate([twice] * (nodes // 16), axis=0) * own_mask
                weights[slot, k * nodes : (k + 1) * nodes, columns] = tall
        total = jnp.dot(basis_ref[0], weights[slot, :nodes], preferred_element_type=F32)
        for k in range(1, 3):
            total = total + jnp.dot(
                basis_ref[k], weights[slot, k * nodes : (k + 1) * nodes], preferred_element_type=F32
            )
        acc[p] = total

    def own_sums(p):
        for at in range(2):
            mine = acc[p, :, at * count : (at + 1) * count]
            total = jnp.sum(mine, axis=1, keepdims=True)
            part[:modes] = jnp.where(lane == 2 * p + at, total, part[:modes])

    def edge_forces(p):
        moved = gathered(p, corner_disp[p], range(own_tiles, own_tiles + ghost_tiles))
        forces = forces_of(moved)
        for at in range(2):
            columns = slice(at * count, (at + 1) * count)
            ends = []
            for k in range(3):
                spread = spread_of(forces, at, k)
                tall = jnp.concatenate([spread] * (ghosts // 8), axis=0) * ghost_mask
                edge_weights[p, k * ghosts : (k + 1) * ghosts, columns] = tall.astype(BF16)
                ends.append(spread * tail_mask)
                total = jnp.sum(tall, axis=1, keepdims=True)
                at_rows = slice(k * ghosts, (k + 1) * ghosts)
                nodal[at_rows] = jnp.where(lane == 2 * p + at, total, nodal[at_rows])
            end = jnp.concatenate(ends + [jnp.zeros((8, count), F32)], axis=0)
            edge_weights[p, tail_at : tail_at + 32, columns] = end.astype(BF16)
            total = jnp.sum(end, axis=1, keepdims=True)
            at_rows = slice(tail_at, tail_at + 32)
            nodal[at_rows] = jnp.where(lane == 2 * p + at, total, nodal[at_rows])

    def whole_product(p, squares):
        result = acc[p] + jnp.dot(ghost[:modes], edge_weights[p], preferred_element_type=F32)
        for at in range(2):
            s = 2 * p + at
            mine = result[:, at * count : (at + 1) * count]
            cols_ref[pl.ds(s, modes, stride=snaps), :] = mine
            norm = jnp.sum(mine * mine, axis=0, keepdims=True)
            squares = jnp.where(row == s, norm, squares)
        return squares

    def each_pair(body):
        if pairs <= 4:
            for p in range(pairs):
                body(p)
        else:
            lax.fori_loop(0, pairs, lambda p, c: (body(p), c)[1], 0)

    others = disp.at[pl.ds(0, params - 1), own_part]
    wait_bytes(others, recv_n)
    each_pair(own_product)
    each_pair(own_sums)

    def flipped(ref):
        return jnp.concatenate(
            [jnp.transpose(ref[t * 128 : (t + 1) * 128])[:snaps] for t in range(ref.shape[0] // 128)],
            axis=1,
        )

    part_p[me_p, :, :wide] = flipped(part)
    wait_bytes(backs, recv_d)

    @pl.when(leading)
    def _():
        for c in range(CHUNKS):
            ghost_copy(c).wait_recv()
            for p in range(params - 1):
                hand_on(p, c).start()

    each_pair(edge_forces)
    part_p[me_p, :, wide:] = flipped(nodal)

    def to_lead():
        return remote(part_p.at[me_p], part_p.at[me_p], send_p, recv_p, dev(me_e, lead))

    @pl.when(jnp.logical_not(leading))
    def _():
        to_lead().start()

    def unfold():
        if half:
            ghost[:half, lanes:tail_at] = ghost_in[:half, :ghosts]
            ghost[half:modes, lanes:tail_at] = ghost_in[: modes - half, ghosts:]

    def to_elem(j):
        to = me_e + (j + 1)
        to = jnp.where(to >= elems, to - elems, to)
        return remote(part_e.at[me_e], part_e.at[me_e], send_e, recv_e, dev(to, lead))

    every_elem = part_e.at[pl.ds(0, elems - 1)]

    def result(p):
        return remote(total_ref, total_ref, send_t.at[p], recv_t, dev(me_e, p))

    row = lax.broadcasted_iota(jnp.int32, (snaps, 128), 0)
    across = lax.broadcasted_iota(jnp.int32, (snaps, 128), 1)

    def finish_norm():
        squares = jnp.zeros((snaps, count), F32)
        if pairs <= 4:
            for p in range(pairs):
                squares = whole_product(p, squares)
        else:
            squares = lax.fori_loop(0, pairs, whole_product, squares)
        norm = jnp.sum(jnp.sqrt(squares), axis=1, keepdims=True)
        norms[me] = jnp.sum(jnp.where(row == across, norm, 0.0), axis=0, keepdims=True)

    @pl.when(jnp.logical_not(leading))
    def _():
        if half:
            wait_bytes(ghost_in.at[pl.ds(0, half)], recv_f.at[0])
        unfold()
        wait_bytes(ghost.at[:, pl.ds(0, lanes)], recv_f.at[1])
        finish_norm()

    @pl.when(leading)
    def _():
        ghost[:modes, :lanes] = ghost_in[half : half + modes]
        unfold()
        wait_bytes(part_p.at[pl.ds(0, params - 1)], recv_p)
        finish_norm()
        chip = part_p[0]
        for p in range(1, params):
            chip = chip + part_p[p]
        force = chip[:, wide:]
        high = force.astype(BF16).astype(F32)
        left = force - high
        mid = left.astype(BF16).astype(F32)
        forces = jnp.concatenate([left - mid, mid, high], axis=0).astype(BF16)
        both = (((1,), (1,)), ((), ()))
        parts = lax.dot_general(forces, ghost[:modes], both, preferred_element_type=F32)
        total = parts[:snaps] + parts[snaps : 2 * snaps] + parts[2 * snaps :]
        part_e[me_e] = chip[:, :wide]
        part_e[me_e, :, :modes] = chip[:, :modes] + total

    @pl.when(jnp.logical_not(climbing & top))
    def _():
        pl.semaphore_wait(known, 1)

    def norm_copy(j):
        return remote(norms.at[me], norms.at[me], send_c, recv_c, other(j))

    @pl.when(leading)
    def _():
        for j in range(FAR):
            to_elem(j).start()

    repeat(devices - 1, lambda j: norm_copy(j).start())

    @pl.when(leading)
    def _():
        repeat(elems - 1 - FAR, lambda j: to_elem(j + FAR).start())
        wait_bytes(every_elem, recv_e)
        total = part_e[0]
        for e in range(1, elems):
            total = total + part_e[e]
        total_ref[...] = total
        for p in range(params - 1):
            result(p).start()

    everyone = norms.at[pl.ds(0, devices - 1)]
    wait_bytes(everyone, recv_c)
    whole = norms[0]
    for d in range(1, devices):
        whole = whole + norms[d]
    diagonal = jnp.where(row == across, jnp.broadcast_to(whole, (snaps, 128)), 0.0)
    row_scale = jnp.sum(diagonal, axis=1, keepdims=True) / elem_total
    inverse_ref[...] = jnp.broadcast_to(1.0 / row_scale, (snaps, count))

    @pl.when(jnp.logical_not(leading))
    def _():
        result(0).wait_recv()

    target_ref[...] = total_ref[:, :modes] / (row_scale * math.sqrt(elem_total))

    wait_bytes(others, send_n)
    wait_bytes(everyone, send_c)

    @pl.when(first)
    def _():
        to_relay().wait_send()

    @pl.when(jnp.logical_not(first))
    def _():
        wait_bytes(backs, send_d)

    @pl.when(relaying)
    def _():
        for p in range(params):
            wait_bytes(relay_disp, send_rd.at[p])
        wait_bytes(relay_ghost, send_rg)

    @pl.when(leading)
    def _():
        wait_bytes(packed, send_g)
        for p in range(params - 1):
            wait_bytes(ghost_in, send_f.at[p])
        wait_bytes(every_elem, send_e)
        for p in range(params - 1):
            result(p).wait_send()

    @pl.when(jnp.logical_not(leading))
    def _():
        to_lead().wait_send()


def finish_kernel(cols_ref, inverse_ref, target_ref, training_hbm, target_hbm, training, sem):
    modes, snaps, count = training.shape
    copies = [pltpu.make_async_copy(target_ref, target_hbm, sem.at[0])]
    copies[0].start()
    inverse = inverse_ref[...][None]
    chunks = sem.shape[0] - 1
    size = modes // chunks
    for c in range(chunks):
        rows = pl.ds(c * size, size)
        piece = cols_ref[c * size * snaps : (c + 1) * size * snaps]
        training[rows] = (piece.reshape(size, snaps, count) * inverse).astype(BF16)
        copies.append(pltpu.make_async_copy(training.at[rows], training_hbm.at[rows], sem.at[c + 1]))
        copies[-1].start()
    for copy in copies:
        copy.wait()


def local(elems, params, coords, basis_rows, connectivity, modulus, stiffness):
    own_snaps, modes = coords.shape
    nodes = basis_rows.shape[2]
    count = connectivity.shape[0]
    snaps = own_snaps * params
    ghosts = nodes // 4
    if ghosts % 128 == 0:
        packed = (round_up(modes, 16), 3 * ghosts)
    else:
        packed = (round_up(modes, 16) + round_up(-(-modes // 2), 16), 2 * ghosts)
    edge = round_up(3 * ghosts + 32, 128)
    tiles = nodes // 128 + -(-ghosts // 128)
    wide = round_up(modes, 128)
    dofs = stiffness.shape[0]
    devices = elems * params
    inner = 4
    pairs = snaps // 2
    dma = pltpu.SemaphoreType.DMA
    vmem = pl.BlockSpec(memory_space=pltpu.VMEM)
    hbm = pl.BlockSpec(memory_space=pltpu.HBM)
    cols, inverse, target = pl.pallas_call(
        functools.partial(kernel, elems, params, inner),
        out_shape=(
            jax.ShapeDtypeStruct((modes * snaps, count), F32),
            jax.ShapeDtypeStruct((snaps, count), F32),
            jax.ShapeDtypeStruct((snaps, modes), F32),
        ),
        in_specs=[hbm] * 5,
        out_specs=(vmem, vmem, vmem),
        scratch_shapes=[
            pltpu.VMEM((own_snaps, modes), BF16),
            pltpu.VMEM((3, modes, nodes), BF16),
            pltpu.VMEM((8, count), jnp.int32),
            pltpu.VMEM((1, count), F32),
            pltpu.VMEM((dofs, dofs), F32),
            pltpu.VMEM(packed, BF16),
            pltpu.VMEM(packed, BF16),
            pltpu.VMEM((round_up(modes, 16), edge), BF16),
            pltpu.VMEM((params, tiles, 3, own_snaps, 128), F32),
            pltpu.VMEM((pairs, dofs, 2 * count), F32),
            pltpu.VMEM((pairs if pairs <= 4 else 1, 3 * nodes, 2 * count), BF16),
            pltpu.VMEM((pairs, edge, 2 * count), BF16),
            pltpu.VMEM((pairs, modes, 2 * count), F32),
            pltpu.VMEM((wide, 128), F32),
            pltpu.VMEM((edge, 128), F32),
            pltpu.VMEM((devices, 1, 128), F32),
            pltpu.VMEM((params, snaps, wide + edge), F32),
            pltpu.VMEM((elems, snaps, wide), F32),
            pltpu.VMEM((snaps, wide), F32),
            pltpu.VMEM((params, tiles - nodes // 128, 3, own_snaps, 128), F32),
            pltpu.VMEM(packed, BF16),
            dma((4,)), dma, dma, dma((CHUNKS,)), dma, dma, dma((params - 1,)), dma((2,)),
            dma, dma, dma, dma((params - 1,)), dma,
            dma((params,)), dma, dma, dma((CHUNKS,)),
            pltpu.SemaphoreType.REGULAR, pltpu.SemaphoreType.REGULAR,
        ],
        compiler_params=pltpu.CompilerParams(
            collective_id=0, has_side_effects=True, vmem_limit_bytes=40 * 1024 * 1024
        ),
    )(*(pltpu.with_memory_space_constraint(x, pltpu.HBM) for x in (
        coords, basis_rows, connectivity.T, modulus[None], stiffness
    )))
    chunks = next(c for c in (4, 3, 2, 1) if modes % c == 0)
    training, target = pl.pallas_call(
        finish_kernel,
        out_shape=(
            jax.ShapeDtypeStruct((modes, snaps, count), BF16),
            jax.ShapeDtypeStruct((snaps, modes), F32),
        ),
        in_specs=[vmem, vmem, vmem],
        out_specs=(hbm, hbm),
        scratch_shapes=[pltpu.VMEM((modes, snaps, count), BF16), dma((chunks + 1,))],
        compiler_params=pltpu.CompilerParams(vmem_limit_bytes=20 * 1024 * 1024),
    )(cols, inverse, target)
    return (jnp.transpose(training, (1, 0, 2)), target)


def solution(mesh):
    in_specs = (
        P("param", None),
        P(None, None, "elem"),
        P(("elem", "param"), None),
        P(("elem", "param")),
        P(),
    )
    out_specs = (P(None, None, ("elem", "param")), P())
    run = functools.partial(local, mesh.shape["elem"], mesh.shape["param"])
    return jax.shard_map(run, mesh=mesh, in_specs=in_specs, out_specs=out_specs, check_vma=False)
```

```python
import functools
import math

import jax
import jax.numpy as jnp
from jax import lax
from jax.experimental import pallas as pl
from jax.experimental.pallas import tpu as pltpu
from jax.sharding import PartitionSpec as P

LOGICAL = pl.DeviceIdType.LOGICAL
F32 = jnp.float32
BF16 = jnp.bfloat16
UNROLL = 64
CHUNKS = 4
FAR = 2


def round_up(value, to):
    return -(-value // to) * to


def repeat(count, body):
    if count <= UNROLL:
        for j in range(count):
            body(j)
    else:
        lax.fori_loop(0, count, lambda j, c: (body(j), c)[1], 0)


def kernel(
    elems, params, inner,
    coords_hbm, basis_hbm, conn_hbm, modulus_hbm, stiff_hbm,
    cols_ref, inverse_ref, target_ref,
    coords_ref, basis_ref, conn_ref, modulus_ref, stiff_ref,
    packed, ghost_in, ghost, disp, corner_disp, weights, edge_weights, acc, part, nodal,
    norms, part_p, part_e, total_ref, relay_disp, relay_ghost,
    load, load_b, send_g, recv_g, recv_d, recv_n, send_f, recv_f,
    recv_c, recv_p, recv_e, send_t, recv_t,
    send_rd, recv_rd, recv_rg, climb, known,
):
    send_d, send_n, send_p, send_e = [load.at[i] for i in range(4)]
    send_c, send_rg = load_b, send_p
    own_snaps, modes = coords_hbm.shape
    dofs = stiff_hbm.shape[0]
    snaps = own_snaps * params
    pairs = snaps // 2
    nodes = basis_hbm.shape[2]
    ghosts = nodes // 4
    count = conn_hbm.shape[1]
    devices = elems * params
    outer = elems // inner
    elem_total = count * devices
    wide, edge = part_e.shape[2], ghost.shape[1]
    own_tiles = nodes // 128
    ghost_tiles = disp.shape[1] - own_tiles
    me_e, me_p = lax.axis_index("elem"), lax.axis_index("param")
    me = me_e * params + me_p
    lead = params - 1
    leading = me_p == lead
    first, last = me_e == 0, me_e == elems - 1
    before = jnp.where(first, elems - 1, me_e - 1)
    relay = (elems // 4 + 2) * params + lead
    relaying = me == relay
    me_o, me_i = lax.div(me_e, inner), lax.rem(me_e, inner)
    bottom, top = me_o == 0, me_o == outer - 1
    guide = inner // 2
    climbing = (me_p == 0) & (me_i == guide)

    def dev(e, p):
        return e * params + p

    def other(j):
        to = me + (j + 1)
        return jnp.where(to >= devices, to - devices, to)

    def signal(semaphore, device):
        pl.semaphore_signal(semaphore, inc=1, device_id=device, device_id_type=LOGICAL)

    def remote(src, dst, send, recv, device):
        return pltpu.make_async_remote_copy(
            src_ref=src, dst_ref=dst, send_sem=send, recv_sem=recv,
            device_id=device, device_id_type=LOGICAL,
        )

    def wait_bytes(ref, semaphore):
        pltpu.make_async_copy(ref, ref, semaphore).wait()

    load_basis = pltpu.make_async_copy(basis_hbm, basis_ref, load_b)
    smalls = [
        pltpu.make_async_copy(src, dst, load.at[i])
        for i, (src, dst) in enumerate([
            (coords_hbm, coords_ref), (conn_hbm, conn_ref),
            (modulus_hbm, modulus_ref), (stiff_hbm, stiff_ref),
        ])
    ]
    for copy in [load_basis] + smalls:
        copy.start()

    barrier = pltpu.get_barrier_semaphore()
    @pl.when(first | last)
    def _():
        signal(barrier, relay)

    @pl.when(relaying)
    def _():
        for p in range(params):
            signal(barrier, dev(elems - 1, p))
            signal(barrier, dev(0, p))

    @pl.when(jnp.logical_not(first))
    def _():
        for p in range(params):
            signal(barrier, dev(me_e - 1, p))

    @pl.when(jnp.logical_not(last))
    def _():
        for p in range(params):
            signal(barrier, dev(me_e + 1, p))

    @pl.when(climbing & jnp.logical_not(bottom))
    def _():
        signal(barrier, dev(me_e - inner, 0))

    @pl.when(climbing & jnp.logical_not(top))
    def _():
        signal(barrier, dev(me_e + inner, 0))

    for j in range(1, params):
        to = me_p + j
        signal(barrier, dev(me_e, jnp.where(to >= params, to - params, to)))

    @pl.when(me_i != guide)
    def _():
        signal(barrier, dev(me_o * inner + guide, 0))

    greeted = params - 1 + jnp.where(first | last, 1, params) + params
    greeted += jnp.where(relaying, 2 * params, 0)
    climbs = (inner - 1) * params + 2 - jnp.where(bottom | top, 1, 0)
    greeted += jnp.where(climbing, climbs, 0)

    part[...] = jnp.zeros_like(part)
    nodal[...] = jnp.zeros_like(nodal)
    tail_at = 3 * ghosts
    for p in range(pairs):
        edge_weights[p, tail_at:] = jnp.zeros((edge - tail_at, 2 * count), BF16)
    for copy in smalls:
        copy.wait()
    coords = coords_ref[...]
    load_basis.wait()
    for k in range(3):
        moved = jnp.dot(coords, basis_ref[k], preferred_element_type=F32)
        moved = moved.astype(BF16).astype(F32)
        for t in range(own_tiles):
            disp[me_p, t, k] = moved[:, t * 128 : (t + 1) * 128]
    rows, lanes = packed.shape
    a_rows = round_up(modes, 16)
    half = rows - a_rows
    if half:
        packed[:half, :ghosts] = basis_ref[2, :half, :ghosts]
        packed[: modes - half, ghosts:] = basis_ref[2, half:, :ghosts]
    for k in range(lanes // ghosts):
        packed[half : half + modes, k * ghosts : (k + 1) * ghosts] = basis_ref[k, :, :ghosts]

    pl.semaphore_wait(barrier, greeted)
    own_part, ghost_part = pl.ds(0, own_tiles), pl.ds(own_tiles, ghost_tiles)
    front = disp.at[me_p, pl.ds(0, ghost_tiles)]
    backs = disp.at[:, ghost_part]

    def ghost_disp(p):
        turn = lax.rem(me_p + p, params)
        return remote(front, disp.at[me_p, ghost_part], send_d, recv_d, dev(before, turn))

    def own_disp(p):
        turn = lax.rem(me_p + p, params)
        mine = disp.at[me_p, own_part]
        return remote(mine, mine, send_n, recv_n, dev(me_e, turn))

    def to_relay():
        return remote(front, relay_disp.at[me_p], send_d, recv_rd, relay)

    def from_relay(p):
        return remote(relay_disp, backs, send_rd.at[p], recv_d, dev(elems - 1, p))

    fore = 2 if half else 0
    rear = CHUNKS - fore
    cuts = [half // 16 * c // fore * 16 for c in range(fore)]
    cuts += [half + a_rows // 16 * c // rear * 16 for c in range(rear + 1)]

    def cut(ref, c):
        return ref.at[pl.ds(cuts[c], cuts[c + 1] - cuts[c])]

    def ghost_copy(c):
        return remote(cut(packed, c), cut(ghost_in, c), send_g, recv_g.at[c], dev(before, lead))

    def ghost_to_relay(c):
        return remote(cut(packed, c), cut(relay_ghost, c), send_g, recv_rg.at[c], relay)

    def ghost_from_relay(c):
        return remote(
            cut(relay_ghost, c), cut(ghost_in, c), send_rg, recv_g.at[c], dev(elems - 1, lead)
        )

    def hand_on(p, c):
        to = cut(ghost_in, c)
        if c >= fore:
            to = ghost.at[pl.ds(cuts[c] - half, cuts[c + 1] - cuts[c]), pl.ds(0, lanes)]
        kind = 0 if c < fore else 1
        return remote(cut(ghost_in, c), to, send_f.at[p], recv_f.at[kind], dev(me_e, p))

    @pl.when(first)
    def _():
        to_relay().start()

    @pl.when(jnp.logical_not(first))
    def _():
        for p in range(params):
            ghost_disp(p).start()

    @pl.when(first & leading)
    def _():
        for c in range(CHUNKS):
            ghost_to_relay(c).start()

    @pl.when(jnp.logical_not(first | relaying) & leading)
    def _():
        for c in range(CHUNKS):
            ghost_copy(c).start()

    for p in range(1, params):
        own_disp(p).start()

    @pl.when(relaying)
    def _():
        wait_bytes(relay_disp, recv_rd)
        for p in range(params):
            from_relay(p).start()
        for c in range(CHUNKS):
            ghost_to_relay(c).wait_recv()
            ghost_from_relay(c).start()
        for c in range(CHUNKS):
            ghost_copy(c).start()

    @pl.when(climbing & jnp.logical_not(bottom))
    def _():
        pl.semaphore_wait(climb, 1)

    @pl.when(climbing & jnp.logical_not(top))
    def _():
        signal(climb, dev(me_e + inner, 0))

    @pl.when(climbing & top)
    def _():
        repeat(devices - 1, lambda j: signal(known, other(j)))

    corners = conn_ref[...]
    base = jnp.min(corners, axis=0, keepdims=True)
    residue = corners % 8
    lane_at = corners % 128
    tile_at = corners // 128
    row8 = lax.broadcasted_iota(jnp.int32, (8, count), 0)
    lane = lax.broadcasted_iota(jnp.int32, (1, 128), 1)
    hits = [residue[a : a + 1] == row8 for a in range(8)]

    def inside(start, height):
        node = start + lax.broadcasted_iota(jnp.int32, (height, count), 0)
        return (node >= base) & (node < base + 8)

    own_rows = lax.broadcasted_iota(jnp.int32, (nodes, count), 0) < nodes - 8
    own_mask = jnp.where(inside(0, nodes) & own_rows, 1.0, 0.0).astype(BF16)
    ghost_mask = jnp.where(inside(nodes, ghosts), 1.0, 0.0)
    tail_mask = jnp.where(inside(nodes - 8, 8), 1.0, 0.0)
    stiff = stiff_ref[...]
    high = stiff.astype(BF16)
    rest = stiff - high.astype(F32)
    mid = rest.astype(BF16)
    low = (rest - mid.astype(F32)).astype(BF16)
    modulus = modulus_ref[...]
    modulus2 = jnp.concatenate([modulus, modulus], axis=1)
    tails = [basis_ref[k, :, nodes - 8 :] for k in range(3)]
    start = tail_at // 128 * 128
    blank = [jnp.zeros((modes, tail_at - start), BF16)] if tail_at > start else []
    after = [jnp.zeros((modes, edge - tail_at - 24), BF16)]
    ghost[:modes, start:] = jnp.concatenate(blank + tails + after, axis=1)

    def gathered(p, found, tiles):
        pieces = []
        for at in range(2):
            s = 2 * p + at
            parts = []
            for k in range(3):
                piece = found[k * 8 : (k + 1) * 8, at * count : (at + 1) * count]
                for t in tiles:
                    line = disp[s // own_snaps, t, k, pl.ds(s % own_snaps, 1), :]
                    got = jnp.take_along_axis(jnp.broadcast_to(line, (8, 128)), lane_at, axis=1)
                    piece = jnp.where(tile_at == t, got, piece)
                parts.append(piece)
            pieces.append(jnp.concatenate(parts, axis=0))
        return jnp.concatenate(pieces, axis=1)

    def forces_of(moved):
        moved16 = moved.astype(BF16)
        linear = jnp.dot(low, moved16, preferred_element_type=F32)
        linear = linear + jnp.dot(mid, moved16, preferred_element_type=F32)
        linear = linear + jnp.dot(high, moved16, preferred_element_type=F32)
        return (modulus2 * (linear + 0.25 * moved * moved * moved)).astype(BF16).astype(F32)

    def spread_of(forces, at, k):
        spread = jnp.zeros((8, count), F32)
        for a in range(8):
            force = forces[k * 8 + a : k * 8 + a + 1, at * count : (at + 1) * count]
            spread = spread + jnp.where(hits[a], force, 0.0)
        return spread.astype(BF16).astype(F32)

    def own_product(p):
        slot = p if weights.shape[0] > 1 else 0
        moved = gathered(p, jnp.zeros((dofs, 2 * count), F32), range(own_tiles))
        corner_disp[p] = moved
        forces = forces_of(moved)
        for at in range(2):
            columns = slice(at * count, (at + 1) * count)
            for k in range(3):
                spread = spread_of(forces, at, k)
                twice = jnp.concatenate([spread, spread], axis=0).astype(BF16)
                tall = jnp.concatenate([twice] * (nodes // 16), axis=0) * own_mask
                weights[slot, k * nodes : (k + 1) * nodes, columns] = tall
        total = jnp.dot(basis_ref[0], weights[slot, :nodes], preferred_element_type=F32)
        for k in range(1, 3):
            total = total + jnp.dot(
                basis_ref[k], weights[slot, k * nodes : (k + 1) * nodes], preferred_element_type=F32
            )
        acc[p] = total

    def own_sums(p):
        for at in range(2):
            mine = acc[p, :, at * count : (at + 1) * count]
            total = jnp.sum(mine, axis=1, keepdims=True)
            part[:modes] = jnp.where(lane == 2 * p + at, total, part[:modes])

    def edge_forces(p):
        moved = gathered(p, corner_disp[p], range(own_tiles, own_tiles + ghost_tiles))
        forces = forces_of(moved)
        for at in range(2):
            columns = slice(at * count, (at + 1) * count)
            ends = []
            for k in range(3):
                spread = spread_of(forces, at, k)
                tall = jnp.concatenate([spread] * (ghosts // 8), axis=0) * ghost_mask
                edge_weights[p, k * ghosts : (k + 1) * ghosts, columns] = tall.astype(BF16)
                ends.append(spread * tail_mask)
                total = jnp.sum(tall, axis=1, keepdims=True)
                at_rows = slice(k * ghosts, (k + 1) * ghosts)
                nodal[at_rows] = jnp.where(lane == 2 * p + at, total, nodal[at_rows])
            end = jnp.concatenate(ends + [jnp.zeros((8, count), F32)], axis=0)
            edge_weights[p, tail_at : tail_at + 32, columns] = end.astype(BF16)
            total = jnp.sum(end, axis=1, keepdims=True)
            at_rows = slice(tail_at, tail_at + 32)
            nodal[at_rows] = jnp.where(lane == 2 * p + at, total, nodal[at_rows])

    def whole_product(p, squares):
        result = acc[p] + jnp.dot(ghost[:modes], edge_weights[p], preferred_element_type=F32)
        for at in range(2):
            s = 2 * p + at
            mine = result[:, at * count : (at + 1) * count]
            cols_ref[pl.ds(s, modes, stride=snaps), :] = mine
            norm = jnp.sum(mine * mine, axis=0, keepdims=True)
            squares = jnp.where(row == s, norm, squares)
        return squares

    def each_pair(body):
        if pairs <= 4:
            for p in range(pairs):
                body(p)
        else:
            lax.fori_loop(0, pairs, lambda p, c: (body(p), c)[1], 0)

    others = disp.at[pl.ds(0, params - 1), own_part]
    wait_bytes(others, recv_n)
    each_pair(own_product)
    each_pair(own_sums)

    def flipped(ref):
        return jnp.concatenate(
            [jnp.transpose(ref[t * 128 : (t + 1) * 128])[:snaps] for t in range(ref.shape[0] // 128)],
            axis=1,
        )

    part_p[me_p, :, :wide] = flipped(part)
    wait_bytes(backs, recv_d)

    @pl.when(leading)
    def _():
        for c in range(CHUNKS):
            ghost_copy(c).wait_recv()
            for p in range(params - 1):
                hand_on(p, c).start()

    each_pair(edge_forces)
    part_p[me_p, :, wide:] = flipped(nodal)

    def to_lead():
        return remote(part_p.at[me_p], part_p.at[me_p], send_p, recv_p, dev(me_e, lead))

    @pl.when(jnp.logical_not(leading))
    def _():
        to_lead().start()

    def unfold():
        if half:
            ghost[:half, lanes:tail_at] = ghost_in[:half, :ghosts]
            ghost[half:modes, lanes:tail_at] = ghost_in[: modes - half, ghosts:]

    def to_elem(j):
        to = me_e + (j + 1)
        to = jnp.where(to >= elems, to - elems, to)
        return remote(part_e.at[me_e], part_e.at[me_e], send_e, recv_e, dev(to, lead))

    every_elem = part_e.at[pl.ds(0, elems - 1)]

    def result(p):
        return remote(total_ref, total_ref, send_t.at[p], recv_t, dev(me_e, p))

    row = lax.broadcasted_iota(jnp.int32, (snaps, 128), 0)
    across = lax.broadcasted_iota(jnp.int32, (snaps, 128), 1)

    def finish_norm():
        squares = jnp.zeros((snaps, count), F32)
        if pairs <= 4:
            for p in range(pairs):
                squares = whole_product(p, squares)
        else:
            squares = lax.fori_loop(0, pairs, whole_product, squares)
        norm = jnp.sum(jnp.sqrt(squares), axis=1, keepdims=True)
        norms[me] = jnp.sum(jnp.where(row == across, norm, 0.0), axis=0, keepdims=True)

    @pl.when(jnp.logical_not(leading))
    def _():
        if half:
            wait_bytes(ghost_in.at[pl.ds(0, half)], recv_f.at[0])
        unfold()
        wait_bytes(ghost.at[:, pl.ds(0, lanes)], recv_f.at[1])
        finish_norm()

    @pl.when(leading)
    def _():
        ghost[:modes, :lanes] = ghost_in[half : half + modes]
        unfold()
        wait_bytes(part_p.at[pl.ds(0, params - 1)], recv_p)
        finish_norm()
        chip = part_p[0]
        for p in range(1, params):
            chip = chip + part_p[p]
        force = chip[:, wide:]
        high = force.astype(BF16).astype(F32)
        left = force - high
        mid = left.astype(BF16).astype(F32)
        forces = jnp.concatenate([left - mid, mid, high], axis=0).astype(BF16)
        both = (((1,), (1,)), ((), ()))
        parts = lax.dot_general(forces, ghost[:modes], both, preferred_element_type=F32)
        total = parts[:snaps] + parts[snaps : 2 * snaps] + parts[2 * snaps :]
        part_e[me_e] = chip[:, :wide]
        part_e[me_e, :, :modes] = chip[:, :modes] + total

    @pl.when(jnp.logical_not(climbing & top))
    def _():
        pl.semaphore_wait(known, 1)

    def norm_copy(j):
        return remote(norms.at[me], norms.at[me], send_c, recv_c, other(j))

    @pl.when(leading)
    def _():
        for j in range(FAR):
            to_elem(j).start()

    repeat(devices - 1, lambda j: norm_copy(j).start())

    @pl.when(leading)
    def _():
        repeat(elems - 1 - FAR, lambda j: to_elem(j + FAR).start())
        wait_bytes(every_elem, recv_e)
        total = part_e[0]
        for e in range(1, elems):
            total = total + part_e[e]
        total_ref[...] = total
        for p in range(params - 1):
            result(p).start()

    everyone = norms.at[pl.ds(0, devices - 1)]
    wait_bytes(everyone, recv_c)
    whole = norms[0]
    for d in range(1, devices):
        whole = whole + norms[d]
    diagonal = jnp.where(row == across, jnp.broadcast_to(whole, (snaps, 128)), 0.0)
    row_scale = jnp.sum(diagonal, axis=1, keepdims=True) / elem_total
    inverse_ref[...] = jnp.broadcast_to(1.0 / row_scale, (snaps, count))

    @pl.when(jnp.logical_not(leading))
    def _():
        result(0).wait_recv()

    target_ref[...] = total_ref[:, :modes] / (row_scale * math.sqrt(elem_total))

    wait_bytes(others, send_n)
    wait_bytes(everyone, send_c)

    @pl.when(first)
    def _():
        to_relay().wait_send()

    @pl.when(jnp.logical_not(first))
    def _():
        wait_bytes(backs, send_d)

    @pl.when(relaying)
    def _():
        for p in range(params):
            wait_bytes(relay_disp, send_rd.at[p])
        wait_bytes(relay_ghost, send_rg)

    @pl.when(leading)
    def _():
        wait_bytes(packed, send_g)
        for p in range(params - 1):
            wait_bytes(ghost_in, send_f.at[p])
        wait_bytes(every_elem, send_e)
        for p in range(params - 1):
            result(p).wait_send()

    @pl.when(jnp.logical_not(leading))
    def _():
        to_lead().wait_send()


def finish_kernel(cols_ref, inverse_ref, target_ref, training_hbm, target_hbm, training, sem):
    modes, snaps, count = training.shape
    copies = [pltpu.make_async_copy(target_ref, target_hbm, sem.at[0])]
    copies[0].start()
    inverse = inverse_ref[...][None]
    chunks = sem.shape[0] - 1
    size = modes // chunks
    for c in range(chunks):
        rows = pl.ds(c * size, size)
        piece = cols_ref[c * size * snaps : (c + 1) * size * snaps]
        training[rows] = (piece.reshape(size, snaps, count) * inverse).astype(BF16)
        copies.append(pltpu.make_async_copy(training.at[rows], training_hbm.at[rows], sem.at[c + 1]))
        copies[-1].start()
    for copy in copies:
        copy.wait()


def local(elems, params, coords, basis_rows, connectivity, modulus, stiffness):
    own_snaps, modes = coords.shape
    nodes = basis_rows.shape[2]
    count = connectivity.shape[0]
    snaps = own_snaps * params
    ghosts = nodes // 4
    if ghosts % 128 == 0:
        packed = (round_up(modes, 16), 3 * ghosts)
    else:
        packed = (round_up(modes, 16) + round_up(-(-modes // 2), 16), 2 * ghosts)
    edge = round_up(3 * ghosts + 32, 128)
    tiles = nodes // 128 + -(-ghosts // 128)
    wide = round_up(modes, 128)
    dofs = stiffness.shape[0]
    devices = elems * params
    inner = 4
    pairs = snaps // 2
    dma = pltpu.SemaphoreType.DMA
    vmem = pl.BlockSpec(memory_space=pltpu.VMEM)
    hbm = pl.BlockSpec(memory_space=pltpu.HBM)
    cols, inverse, target = pl.pallas_call(
        functools.partial(kernel, elems, params, inner),
        out_shape=(
            jax.ShapeDtypeStruct((modes * snaps, count), F32),
            jax.ShapeDtypeStruct((snaps, count), F32),
            jax.ShapeDtypeStruct((snaps, modes), F32),
        ),
        in_specs=[hbm] * 5,
        out_specs=(vmem, vmem, vmem),
        scratch_shapes=[
            pltpu.VMEM((own_snaps, modes), BF16),
            pltpu.VMEM((3, modes, nodes), BF16),
            pltpu.VMEM((8, count), jnp.int32),
            pltpu.VMEM((1, count), F32),
            pltpu.VMEM((dofs, dofs), F32),
            pltpu.VMEM(packed, BF16),
            pltpu.VMEM(packed, BF16),
            pltpu.VMEM((round_up(modes, 16), edge), BF16),
            pltpu.VMEM((params, tiles, 3, own_snaps, 128), F32),
            pltpu.VMEM((pairs, dofs, 2 * count), F32),
            pltpu.VMEM((pairs if pairs <= 4 else 1, 3 * nodes, 2 * count), BF16),
            pltpu.VMEM((pairs, edge, 2 * count), BF16),
            pltpu.VMEM((pairs, modes, 2 * count), F32),
            pltpu.VMEM((wide, 128), F32),
            pltpu.VMEM((edge, 128), F32),
            pltpu.VMEM((devices, 1, 128), F32),
            pltpu.VMEM((params, snaps, wide + edge), F32),
            pltpu.VMEM((elems, snaps, wide), F32),
            pltpu.VMEM((snaps, wide), F32),
            pltpu.VMEM((params, tiles - nodes // 128, 3, own_snaps, 128), F32),
            pltpu.VMEM(packed, BF16),
            dma((4,)), dma, dma, dma((CHUNKS,)), dma, dma, dma((params - 1,)), dma((2,)),
            dma, dma, dma, dma((params - 1,)), dma,
            dma((params,)), dma, dma((CHUNKS,)),
            pltpu.SemaphoreType.REGULAR, pltpu.SemaphoreType.REGULAR,
        ],
        compiler_params=pltpu.CompilerParams(
            collective_id=0, has_side_effects=True, vmem_limit_bytes=40 * 1024 * 1024
        ),
    )(*(pltpu.with_memory_space_constraint(x, pltpu.HBM) for x in (
        coords, basis_rows, connectivity.T, modulus[None], stiffness
    )))
    chunks = next(c for c in (4, 3, 2, 1) if modes % c == 0)
    training, target = pl.pallas_call(
        finish_kernel,
        out_shape=(
            jax.ShapeDtypeStruct((modes, snaps, count), BF16),
            jax.ShapeDtypeStruct((snaps, modes), F32),
        ),
        in_specs=[vmem, vmem, vmem],
        out_specs=(hbm, hbm),
        scratch_shapes=[pltpu.VMEM((modes, snaps, count), BF16), dma((chunks + 1,))],
        compiler_params=pltpu.CompilerParams(vmem_limit_bytes=20 * 1024 * 1024),
    )(cols, inverse, target)
    return (jnp.transpose(training, (1, 0, 2)), target)


def solution(mesh):
    in_specs = (
        P("param", None),
        P(None, None, "elem"),
        P(("elem", "param"), None),
        P(("elem", "param")),
        P(),
    )
    out_specs = (P(None, None, ("elem", "param")), P())
    run = functools.partial(local, mesh.shape["elem"], mesh.shape["param"])
    return jax.shard_map(run, mesh=mesh, in_specs=in_specs, out_specs=out_specs, check_vma=False)
```
